256 devices in a mesh: dp: 8 (over x, core), expert: 8 (over z), mp: 4 (over y).
Axes of the slice: x: 4, y: 4, z: 8, core: 2. Of those that a mesh axis runs over, the one named last changes fastest.
Arguments:
- tokens: bfloat16 [2048, 4096], P('dp', ('expert', 'mp')), may hold values from -6 to 6
- expert_index: int32 [2048, 2], P('dp'), may hold values from 0 to 7, as said below
- slot_index: int32 [2048, 2], P('dp'), may hold values from 0 to 95, as said below
- norm_gain: float32 [4096], P(('expert', 'mp')), may hold values from 0.1 to 1.9
- router_weight: bfloat16 [8, 4096], P(None, ('expert', 'mp')), may hold values from -8 to 8
- gate_weight: bfloat16 [8, 7168, 4096], P('expert', ('dp', 'mp')), may hold values from -0.09375 to 0.09375
- up_weight: bfloat16 [8, 7168, 4096], P('expert', ('dp', 'mp')), may hold values from -0.09375 to 0.09375
- down_weight: bfloat16 [8, 7168, 4096], P('expert', ('dp', 'mp')), may hold values from -0.125 to 0.125
- final_gain: float32 [4096], replicated, may hold values from 0.1 to 1.9
- head_weight: bfloat16 [16384, 4096], P(('expert', 'mp')), may hold values from -8 to 8
Outputs:
- layer_out: bfloat16 [2048, 4096], P('dp', ('expert', 'mp'))
- head_logsum: float32 [2048], P('dp')
- router_penalty: float32 [], replicated
- head_penalty: float32 [], replicated
The draws below stay inside these ranges and needn't reach their ends.
Inputs may be any that keep to these rules, and one draw needn't show every extreme that they name: `expert_index`: each row names 2 different experts. In each aligned block of 256 rows every expert is named at least once and at most 96 times; in every block two experts are named exactly 96 times, and one of them is the same expert in all blocks. `slot_index`: within each aligned block of 256 rows, the choices that name one expert hold the slots 0, 1, 2, ... in the order of rows, and within a row in the order of choices.
All inputs are finite; a program needn't handle non-finite values.
Results may differ from the reference program's by a relative error of at most 0.01115.
Values may be sent and summed in bfloat16 or wider, within the bound.
A program may use at most 128 MiB of HBM per device.

```python
import math
import jax
import jax.numpy as jnp
from jax import lax

D = 4096
FF = 7168
VOCAB = 16384
TOP = 2
TOK_DP = 256
EXPERTS = 8
TOKENS = 2048
CAPACITY = 96
SLOTS = 768


def routing_tables(key):
    blocks = TOKENS // TOK_DP
    remain = 2 * TOK_DP - 2 * CAPACITY
    others = EXPERTS - 2
    base_count = remain // others
    extra_count = remain % others
    full_expert = jax.random.randint(jax.random.fold_in(key, 5), (), 0, EXPERTS)

    def one_block(block_key):
        key_order = jax.random.fold_in(block_key, 1)
        key_moved = jax.random.fold_in(block_key, 2)
        key_shuffle = jax.random.fold_in(block_key, 3)
        key_swap = jax.random.fold_in(block_key, 4)
        rest_order = 1 + jax.random.permutation(key_order, EXPERTS - 1).astype(jnp.int32)
        rank_expert = (full_expert + jnp.concatenate([jnp.zeros((1,), jnp.int32), rest_order])) % EXPERTS
        rank_ids = jnp.arange(others, dtype=jnp.int32)
        counts_rest = base_count + (rank_ids < extra_count).astype(jnp.int32)
        moved_count = jax.random.randint(key_moved, (others,), 0, base_count // 4 + 1)
        counts_rest = counts_rest - moved_count + jnp.roll(moved_count, 1)
        counts = jnp.concatenate([jnp.full((2,), CAPACITY, jnp.int32), counts_rest])
        bounds = jnp.cumsum(counts)
        places = jnp.arange(2 * TOK_DP, dtype=jnp.int32)
        rank_of = jnp.sum((places[:, None] >= bounds[None, :]).astype(jnp.int32), axis=1)
        labels = rank_expert[rank_of]
        choice_pairs = jnp.stack([labels[:TOK_DP], labels[TOK_DP:]], axis=1)
        shuffle = jax.random.permutation(key_shuffle, TOK_DP)
        choice_pairs = choice_pairs[shuffle]
        swap_order = jax.random.randint(key_swap, (TOK_DP, 1), 0, 2)
        choice_pairs = jnp.where(swap_order == 1, choice_pairs[:, ::-1], choice_pairs)
        flat_pairs = choice_pairs.reshape(-1)
        hit_table = (flat_pairs[:, None] == jnp.arange(EXPERTS, dtype=jnp.int32)[None, :]).astype(jnp.int32)
        running = jnp.cumsum(hit_table, axis=0)
        slot_table = jnp.sum(hit_table * running, axis=1) - 1
        return (choice_pairs.astype(jnp.int32), slot_table.reshape(TOK_DP, 2).astype(jnp.int32))
    block_keys = jax.random.split(jax.random.fold_in(key, 7), blocks)
    chosen, slotted = jax.vmap(one_block)(block_keys)
    return (chosen.reshape(TOKENS, 2), slotted.reshape(TOKENS, 2))


def draw_expert_index(key, part):
    return routing_tables(jax.random.fold_in(key, 11))[0]


def draw_slot_index(key, part):
    return routing_tables(jax.random.fold_in(key, 11))[1]


def drawn_rows(key, rows, width, scale):
    base_key = jax.random.fold_in(key, 1)
    values = jax.random.normal(base_key, (rows, width), jnp.float32) * scale
    return jnp.clip(values, -8.0, 8.0).astype(jnp.bfloat16)


def draw_router_weight(key, part):
    return drawn_rows(jax.random.fold_in(key, 21), EXPERTS, D, 1.0 / math.sqrt(D))


def draw_head_weight(key, part):
    return drawn_rows(jax.random.fold_in(key, 31), VOCAB, D, 3.0 / math.sqrt(D))


def with_spikes(drawn, own_key, source, target, blocks, factor):
    owner, partner = [(jnp.arange(drawn.shape[dim]) // (drawn.shape[dim] // blocks)).reshape([-1 if axis == dim else 1 for axis in range(drawn.ndim)]) for dim in (source, target)]
    chosen = jax.random.permutation(own_key, blocks)[partner]
    strong = (owner == chosen) | (owner == (partner + blocks // 2) % blocks)
    return jnp.where(strong, factor * drawn, drawn)


def steps_of(own_key, extent, pieces, least, top_value):
    level, own = 1.0, jax.random.fold_in(own_key, 6)
    for axis_at, parts in pieces:
        draws = jnp.exp(jax.random.uniform(jax.random.fold_in(own, axis_at), (parts,), jnp.float32, least / len(pieces), top_value / len(pieces)))
        level = level * jnp.repeat(draws, extent[axis_at] // parts).reshape([-1 if axis == axis_at else 1 for axis in range(len(extent))])
    return level


def noise(own_key, dims, deviation, bound, cuts=(), held_as=jnp.bfloat16):
    array = jax.random.normal(own_key, dims, jnp.float32) * deviation
    if len(cuts) > 0:
        array = steps_of(own_key, dims, cuts, -0.22, 0.18) * array
    return jnp.clip(array, min=-bound, max=bound).astype(held_as)


def noise_with(key, shape, scale, limit, shards, heavy, kind=jnp.bfloat16):
    values = scale * jax.random.normal(key, shape, jnp.float32)
    if shards:
        values = values * steps_of(key, shape, shards, -0.22, 0.18)
    return jnp.clip(with_spikes(values, jax.random.fold_in(key, 3), *heavy), -limit, limit).astype(kind)


def setup_inputs(seed: int = 0) -> dict:
    arg_keys = jax.random.split(jax.random.key(seed), 11)
    return {
        "tokens": noise(arg_keys[0], (TOKENS, D), 1.0, 6.0, ((0, 8), (1, 32))),
        "expert_index": draw_expert_index(jax.random.fold_in(arg_keys[10], 71), 0),
        "slot_index": draw_slot_index(jax.random.fold_in(arg_keys[10], 71), 0),
        "norm_gain": jnp.clip(1.0 + 0.18 * jax.random.normal(arg_keys[3], (D,), jnp.float32), 0.1, 1.9),
        "router_weight": draw_router_weight(jax.random.fold_in(arg_keys[10], 71), 0),
        "gate_weight": noise(arg_keys[5], (EXPERTS, FF, D), D ** -0.5, 0.09375, ((0, 8), (1, 32))),
        "up_weight": noise(arg_keys[6], (EXPERTS, FF, D), D ** -0.5, 0.09375, ((0, 8), (1, 32))),
        "down_weight": noise_with(arg_keys[7], (EXPERTS, FF, D), FF ** -0.5, 0.125, ((0, 8), (1, 32)), (1, 2, 32, 2.75)),
        "final_gain": jnp.clip(1.0 + 0.18 * jax.random.normal(arg_keys[8], (D,), jnp.float32), 0.1, 1.9),
        "head_weight": draw_head_weight(jax.random.fold_in(arg_keys[10], 71), 0),
    }


epsilon = 1e-05

def run_expert(operands):
    slot_rows, gate_matrix, up_matrix, down_matrix = operands
    gate_value = jnp.dot(slot_rows, gate_matrix.T, preferred_element_type=jnp.float32)
    up_value = jnp.dot(slot_rows, up_matrix.T, preferred_element_type=jnp.float32)
    hidden = (jax.nn.silu(gate_value) * up_value).astype(jnp.bfloat16)
    return jnp.dot(hidden, down_matrix, preferred_element_type=jnp.float32).astype(jnp.bfloat16)

def reference(tokens, expert_index, slot_index, norm_gain, router_weight, gate_weight, up_weight, down_weight, final_gain, head_weight):
    tokens_float = tokens.astype(jnp.float32)
    inverse = lax.rsqrt(lax.optimization_barrier(jnp.mean(tokens_float * tokens_float, axis=1)) + epsilon)
    normed = tokens_float * inverse[:, None] * norm_gain[None, :]
    normed_rows = normed.astype(jnp.bfloat16)
    router_logits = jnp.dot(normed, router_weight.astype(jnp.float32).T, precision=lax.Precision.HIGHEST)
    router_logsum = jax.nn.logsumexp(router_logits, axis=1)
    picked = jnp.take_along_axis(router_logits, expert_index, axis=1)
    gate_weights = jax.nn.softmax(picked, axis=1)
    shard_number = jnp.arange(TOKENS, dtype=jnp.int32) // TOK_DP
    position = shard_number[:, None] * CAPACITY + slot_index
    buffer = jnp.zeros((EXPERTS, SLOTS, D), jnp.bfloat16)
    buffer = buffer.at[expert_index.reshape(-1), position.reshape(-1)].set(jnp.repeat(normed_rows, TOP, axis=0))
    outputs = lax.map(run_expert, (buffer, gate_weight, up_weight, down_weight))
    picked_rows = outputs[expert_index, position]
    combined = lax.optimization_barrier(jnp.sum(gate_weights[:, :, None] * picked_rows.astype(jnp.float32), axis=1))
    layer_out = (tokens_float + combined).astype(jnp.bfloat16)
    layer_float = layer_out.astype(jnp.float32)
    head_scale = lax.rsqrt(lax.optimization_barrier(jnp.mean(layer_float * layer_float, axis=1)) + epsilon)
    head_in = (layer_float * head_scale[:, None] * final_gain[None, :]).astype(jnp.bfloat16)
    logits = jnp.dot(head_in, head_weight.T, preferred_element_type=jnp.float32)
    head_logsum = jax.nn.logsumexp(logits, axis=1)
    return (layer_out, head_logsum, jnp.mean(router_logsum * router_logsum), jnp.mean(head_logsum * head_logsum))
```

```python
import jax
import jax.numpy as jnp
from jax import lax
from jax.experimental import pallas as pl
from jax.experimental.pallas import tpu as pltpu
from jax.sharding import PartitionSpec as P

F32 = jnp.float32
BF16 = jnp.bfloat16
EPSILON = 1e-05
LAST = (((1,), (1,)), ((), ()))
EXACT = lax.Precision.HIGHEST

NX, NY, NZ = 4, 4, 8
CAP = 96
TOK = 256
LANE = 128
HID = 224
HID2 = 2 * HID
WIDTH = LANE * NY * NZ
ROWS = NX * CAP
SEMS = 256
CUT_A, CUT_B = 144, 256
SUB_A, SUB_B = 80, 208


def kernel(
    tk, ei, si, ng, rw, fg, gw_h, uw_h, dw_h, hw_h,
    out_ref, lse_ref, rp_ref, hp_ref,
    gw, uw, dw, hw, ls, xs, acc_g, acc_u, hid, ps, ra_a, rb_a, ra_b, rb_b, sa, sb,
    ra2_a, rb2_a, ra2_b, rb2_b, fin, rx, chi, clo, hs, acc_h,
    zbuf, ybuf, ibuf, mzbuf, mybuf, pbuf, ssem, rsem, lsem,
):
    d = lax.axis_index("dp")
    e = lax.axis_index("expert")
    m = lax.axis_index("mp")
    x = d // 2
    c = d % 2
    coord = {"x": x, "y": m, "z": e}
    size = {"x": NX, "y": NY, "z": NZ}

    def at(axis, step):
        return (coord[axis] + step + size[axis]) % size[axis]

    def device(axis, step):
        if axis == "x":
            return {"dp": at("x", step) * 2 + c, "expert": e, "mp": m}
        if axis == "y":
            return {"dp": d, "expert": e, "mp": at("y", step)}
        return {"dp": d, "expert": at("z", step), "mp": m}

    def core(step):
        return {"dp": at("x", step) * 2 + (1 - c), "expert": e, "mp": m}

    ids = {}
    sent = []

    def remote(tag, src, dst, dev):
        number = ids.setdefault(tag, len(ids))
        return pltpu.make_async_remote_copy(
            src_ref=src, dst_ref=dst, send_sem=ssem.at[number], recv_sem=rsem.at[number],
            device_id=dev, device_id_type=pl.DeviceIdType.MESH,
        )

    def send(tag, src, dst, dev):
        copy = remote(tag, src, dst, dev)
        copy.start()
        sent.append(copy)

    def wait(tag, ref):
        remote(tag, ref, ref, device("y", 1)).wait_recv()

    loads = [
        pltpu.make_async_copy(gw_h, gw.at[pl.ds(0, HID)], lsem.at[0]),
        pltpu.make_async_copy(uw_h, uw.at[pl.ds(0, HID)], lsem.at[1]),
        pltpu.make_async_copy(dw_h, dw.at[pl.ds(0, HID)], lsem.at[2]),
        pltpu.make_async_copy(hw_h, hw, lsem.at[3]),
    ]
    for load in loads:
        load.start()
    barrier = pltpu.get_barrier_semaphore()
    partners = [device("z", k) for k in range(1, NZ)]
    partners += [device("y", k) for k in range(1, NY)]
    partners += [device("x", k) for k in range(1, NX)]
    partners += [core(k) for k in range(NX)]
    for partner in partners:
        pl.semaphore_signal(
            barrier, inc=1, device_id=partner, device_id_type=pl.DeviceIdType.MESH
        )

    t32 = tk[...].astype(F32)
    gained = (t32 * ng[...]).astype(BF16)
    flat0 = ei[0:1, :] * CAP + si[0:1, :]
    flat1 = ei[1:2, :] * CAP + si[1:2, :]
    slot_iota = lax.broadcasted_iota(jnp.int32, (CAP, TOK), 0)
    for ex in range(NZ):
        rows = slot_iota + ex * CAP
        choose = jnp.where((rows == flat0) | (rows == flat1), 1.0, 0.0).astype(BF16)
        ls[ex] = jnp.dot(choose, gained, preferred_element_type=F32).astype(BF16)
    router_gained = rw[...].astype(F32) * ng[...]
    zbuf[e, 0:8, :] = lax.dot_general(
        router_gained, t32, LAST, precision=EXACT, preferred_element_type=F32
    )
    ones8 = jnp.ones((8, LANE), F32)
    zbuf[e, 8:16, :] = lax.dot_general(
        ones8, t32 * t32, LAST, precision=EXACT, preferred_element_type=F32
    )
    xs[m, x, e] = ls[e]

    pl.semaphore_wait(barrier, len(partners))
    for k in (4, 3, 5, 2, 6, 1, 7):
        send(("slots", k), ls.at[at("z", k)], xs.at[m, x, e], device("z", k))
    for k in range(1, NZ):
        send(("router z", k), zbuf.at[e], zbuf.at[e], device("z", k))
    for number, (load, weight) in enumerate(zip(loads, (gw, uw, dw))):
        load.wait()
        send(("weight", number), weight.at[pl.ds(0, HID)], weight.at[pl.ds(HID, HID)], core(0))
    loads[3].wait()

    def ring(rounds, start, tag, axis, view):
        half = size[axis] // 2

        def begin():
            send((tag, "+", 1), view(coord[axis]), view(coord[axis]), device(axis, 1))
            send((tag, "-", 1), view(coord[axis]), view(coord[axis]), device(axis, -1))

        def step(k):
            for sign, toward, part in (("+", 1, 0), ("-", -1, 1)):
                source = at(axis, -toward * k)
                wait((tag, sign, k), view(source))
                if k < half - 1:
                    unit = view(source)
                else:
                    unit = view(source, part)
                send((tag, sign, k + 1), unit, unit, device(axis, toward))

        def finish():
            source = at(axis, half)
            wait((tag, "+", half), view(source, 0))
            wait((tag, "-", half), view(source, 1))

        rounds.setdefault(start, []).append(begin)
        for k in range(1, half):
            rounds.setdefault(start + k, []).append(lambda k=k: step(k))
        rounds.setdefault(start + half, []).append(finish)

    def play(rounds, number):
        for event in rounds.get(number, []):
            event()

    def slab(yy, xx, first):
        def view(part=None):
            if part is None:
                return xs.at[yy, xx, pl.ds(first, 4)]
            return xs.at[yy, xx, pl.ds(first + 2 * part, 2)]
        return view

    gather = {}
    ring(gather, 0, "ga x", "x", lambda s, p=None: slab(m, s, 0)(p))
    ring(gather, 0, "gb y", "y", lambda s, p=None: slab(s, x, 4)(p))
    for step_, start in ((2, 2), (1, 1), (-1, 1), (0, 0)):
        ring(gather, start, ("ga y", step_), "y",
             lambda s, p=None, t=step_: slab(s, at("x", t), 0)(p))
        ring(gather, start, ("gb x", step_), "x",
             lambda s, p=None, t=step_: slab(at("y", t), s, 4)(p))

    for k in range(1, NZ):
        wait(("slots", k), xs.at[m, x, at("z", -k)])
    play(gather, 0)

    for k in range(1, NZ):
        wait(("router z", k), zbuf.at[at("z", -k)])
    total = zbuf[0]
    for k in range(1, NZ):
        total = total + zbuf[k]
    ybuf[m] = total
    for k in range(1, NY):
        send(("router y", k), ybuf.at[m], ybuf.at[m], device("y", k))

    @pl.loop(0, 512 // 16)
    def _(i):
        part = pl.ds(pl.multiple_of(i * 16, 16), 16)
        hw[part, :] = (hw[part, :].astype(F32) * fg[...]).astype(BF16)

    play(gather, 1)

    for k in range(1, NY):
        wait(("router y", k), ybuf.at[at("y", -k)])
    total = ((ybuf[0] + ybuf[1]) + ybuf[2]) + ybuf[3]
    inverse8 = lax.rsqrt(total[8:16] / WIDTH + EPSILON)
    logits = total[0:8] * inverse8
    expert_iota = lax.broadcasted_iota(jnp.int32, (8, TOK), 0)
    place = slot_iota + e * CAP
    mine = jnp.where((place == flat0) | (place == flat1), 1.0, 0.0)
    mine = jnp.concatenate([mine, jnp.zeros((LANE - CAP, TOK), F32)], axis=0)
    ibuf[x] = lax.dot_general(
        inverse8, mine, LAST, precision=EXACT, preferred_element_type=F32
    )
    for k in range(1, NX):
        send(("inverse", k), ibuf.at[x], ibuf.at[x], device("x", k))

    play(gather, 2)

    top = jnp.max(logits, axis=0, keepdims=True)
    router_logsum = top + jnp.log(jnp.sum(jnp.exp(logits - top), axis=0, keepdims=True))
    picked0 = jnp.sum(jnp.where(expert_iota == ei[0:1, :], logits, 0.0), axis=0, keepdims=True)
    picked1 = jnp.sum(jnp.where(expert_iota == ei[1:2, :], logits, 0.0), axis=0, keepdims=True)
    higher = jnp.maximum(picked0, picked1)
    power0 = jnp.exp(picked0 - higher)
    power1 = jnp.exp(picked1 - higher)
    weight0 = power0 / (power0 + power1)
    weight1 = power1 / (power0 + power1)
    chunk_iota = lax.broadcasted_iota(jnp.int32, (LANE, TOK), 0)
    for j in range(NZ * CAP // LANE):
        rows = chunk_iota + j * LANE
        mixed = jnp.where(rows == flat0, weight0, 0.0) + jnp.where(rows == flat1, weight1, 0.0)
        mixed = mixed.T
        high = mixed.astype(BF16)
        chi[:, j * LANE:(j + 1) * LANE] = high
        clo[:, j * LANE:(j + 1) * LANE] = (mixed - high.astype(F32)).astype(BF16)
    acc_g[...] = jnp.zeros_like(acc_g)
    acc_u[...] = jnp.zeros_like(acc_u)

    play(gather, 3)
    for number, weight in enumerate((gw, uw, dw)):
        wait(("weight", number), weight.at[pl.ds(HID, HID)])
    for k in range(1, NX):
        wait(("inverse", k), ibuf.at[at("x", -k)])
    play(gather, 4)

    def columns(weight, ex, yy):
        return weight[:, pl.ds(pl.multiple_of((ex * NY + yy) * LANE, LANE), LANE)]

    @pl.loop(0, NY)
    def _(yy):
        held = jnp.concatenate(
            [xs[yy, :, ex].reshape(ROWS, LANE) for ex in range(NZ)], axis=1
        )
        for acc, weight in ((acc_g, gw), (acc_u, uw)):
            against = jnp.concatenate([columns(weight, ex, yy) for ex in range(NZ)], axis=1)
            acc[...] += lax.dot_general(held, against, LAST, preferred_element_type=F32)

    for xx in range(NX):
        rows = pl.ds(xx * CAP, CAP)
        scale = jnp.broadcast_to(ibuf[xx, 0:1, :], (LANE, LANE)).T[0:CAP, 0:1]
        gate_value = acc_g[rows, :] * scale
        up_value = acc_u[rows, :] * scale
        hid[rows, :] = (gate_value / (1.0 + jnp.exp(-gate_value)) * up_value).astype(BF16)

    def down(yy, first):
        against = jnp.concatenate([columns(dw, first + j, yy) for j in range(4)], axis=1)
        product = jnp.dot(hid[...], against, preferred_element_type=F32).astype(BF16)
        for j in range(4):
            for xx in range(NX):
                ps[yy, xx, first + j] = product[
                    xx * CAP:(xx + 1) * CAP, j * LANE:(j + 1) * LANE
                ]

    def reduce_first(tag, axis, view, near):
        send((tag, "+", 1), view(at(axis, 2), 0), near.at[0], device(axis, 1))
        send((tag, "-", 1), view(at(axis, 2), 1), near.at[1], device(axis, -1))

    def add_into(target, source):
        target[...] = (target[...].astype(F32) + source[...].astype(F32)).astype(BF16)

    def reduce_second(tag, axis, view, near, far):
        wait((tag, "+", 1), near.at[0])
        add_into(view(at(axis, 1), 0), near.at[0])
        send((tag, "+", 2), view(at(axis, 1)), far.at[0], device(axis, 1))
        wait((tag, "-", 1), near.at[1])
        add_into(view(at(axis, -1), 1), near.at[1])
        send((tag, "-", 2), view(at(axis, -1)), far.at[1], device(axis, -1))

    def reduce_last(tag, view, far, into):
        wait((tag, "+", 2), far.at[0])
        wait((tag, "-", 2), far.at[1])
        into[...] = (
            view[...].astype(F32) + far[0].astype(F32) + far[1].astype(F32)
        ).astype(BF16)

    def part_a(yy, xx, part=None):
        if part is None:
            return ps.at[yy, xx, pl.ds(0, 4)]
        return ps.at[yy, xx, pl.ds(2 * part, 2)]

    def part_b(yy, xx, part=None):
        if part is None:
            return ps.at[yy, xx, pl.ds(4, 4)]
        return ps.at[yy, xx, pl.ds(4 + 2 * part, 2)]

    order = (2, 1, -1, 0)

    def a_view(t):
        return lambda s, p=None: part_a(s, at("x", t), p)

    def b_view(t):
        return lambda s, p=None: part_b(at("y", t), s, p)

    down(at("y", 2), 0)
    for i, t in enumerate(order):
        reduce_first(("ra y", t), "y", a_view(t), ra_a.at[i])

    @pl.loop(0, NY)
    def _(k):
        down((m + 2 + k) % NY, 4)

    for i, t in enumerate(order):
        reduce_first(("rb x", t), "x", b_view(t), ra_b.at[i])

    @pl.loop(1, NY)
    def _(k):
        down((m + 2 + k) % NY, 0)

    for i, t in enumerate(order):
        reduce_second(("ra y", t), "y", a_view(t), ra_a.at[i], rb_a.at[i])
        reduce_second(("rb x", t), "x", b_view(t), ra_b.at[i], rb_b.at[i])

    def sa_view(s, p=None):
        return sa.at[s] if p is None else sa.at[s, pl.ds(2 * p, 2)]

    def sb_view(s, p=None):
        return sb.at[s] if p is None else sb.at[s, pl.ds(2 * p, 2)]

    for i, t in enumerate(order):
        reduce_last(("ra y", t), a_view(t)(m), rb_a.at[i], sa.at[at("x", t)])
        if t == 2:
            reduce_first("ra x", "x", sa_view, ra2_a)
        reduce_last(("rb x", t), b_view(t)(x), rb_b.at[i], sb.at[at("y", t)])
        if t == 2:
            reduce_first("rb y", "y", sb_view, ra2_b)
        if t == -1:
            reduce_second("ra x", "x", sa_view, ra2_a, rb2_a)
            reduce_second("rb y", "y", sb_view, ra2_b, rb2_b)
    reduce_last("ra x", sa_view(x), rb2_a, fin.at[pl.ds(0, 4)])
    reduce_last("rb y", sb_view(m), rb2_b, fin.at[pl.ds(4, 4)])

    for k in (4, 3, 5, 2, 6, 1, 7):
        send(("back", k), fin.at[at("z", k)], rx.at[e], device("z", k))
    rx[e] = fin[e]
    for k in (1, 7, 2, 6, 3, 5, 4):
        wait(("back", k), rx.at[at("z", -k)])
    outputs = rx[...].reshape(NZ * CAP, LANE)
    combined = jnp.dot(chi[...], outputs, preferred_element_type=F32)
    combined += jnp.dot(clo[...], outputs, preferred_element_type=F32)
    layer_out = (tk[...].astype(F32) + combined).astype(BF16)
    out_ref[...] = layer_out
    hs[m, e] = layer_out

    def rows_a(yy, zz, part=None):
        if part is None:
            return hs.at[yy, zz, pl.ds(0, CUT_A)]
        return hs.at[yy, zz, pl.ds(0, SUB_A)] if part == 0 else hs.at[
            yy, zz, pl.ds(SUB_A, CUT_A - SUB_A)]

    def rows_b(yy, zz, part=None):
        if part is None:
            return hs.at[yy, zz, pl.ds(CUT_A, CUT_B - CUT_A)]
        return hs.at[yy, zz, pl.ds(CUT_A, SUB_B - CUT_A)] if part == 0 else hs.at[
            yy, zz, pl.ds(SUB_B, CUT_B - SUB_B)]

    head = {}
    ring(head, 0, "ha z", "z", lambda s, p=None: rows_a(m, s, p))
    ring(head, 0, "hb y", "y", lambda s, p=None: rows_b(s, e, p))
    for start, steps in ((4, (4,)), (3, (3, -3)), (2, (2, -2)), (1, (1, -1)), (0, (0,))):
        for t in steps:
            ring(head, start, ("ha y", t), "y", lambda s, p=None, t=t: rows_a(s, at("z", t), p))
        if start <= 2:
            for t in {2: (2,), 1: (1, -1), 0: (0,)}[start]:
                ring(head, start, ("hb z", t), "z",
                     lambda s, p=None, t=t: rows_b(at("y", t), s, p))
    for number in range(max(head) + 1):
        play(head, number)

    acc_h[...] = jnp.zeros_like(acc_h)
    acc_h2 = acc_h

    @pl.loop(0, NY)
    def _(yy):
        held = jnp.concatenate([hs[yy, zz] for zz in range(NZ)], axis=1)
        against = jnp.concatenate([columns(hw, zz, yy) for zz in range(NZ)], axis=1)
        acc_h2[0:512, :] += lax.dot_general(against, held, LAST, preferred_element_type=F32)
        squares = jnp.zeros((TOK, LANE), F32)
        for zz in range(NZ):
            block = hs[yy, zz].astype(F32)
            squares = squares + block * block
        acc_h2[512:520, :] += lax.dot_general(
            ones8, squares, LAST, precision=EXACT, preferred_element_type=F32
        )

    head_scale = lax.rsqrt(acc_h[512:513, :] / WIDTH + EPSILON)
    vocab = acc_h[0:512, :] * head_scale
    vocab_max = jnp.max(vocab, axis=0, keepdims=True)
    vocab_sum = jnp.sum(jnp.exp(vocab - vocab_max), axis=0, keepdims=True)

    def merge(pairs):
        top = pairs[0][0]
        for pair in pairs[1:]:
            top = jnp.maximum(top, pair[0])
        whole = pairs[0][1] * jnp.exp(pairs[0][0] - top)
        for pair in pairs[1:]:
            whole = whole + pair[1] * jnp.exp(pair[0] - top)
        return top, whole

    mzbuf[e, 0:1, :] = vocab_max
    mzbuf[e, 1:2, :] = vocab_sum
    for k in (4, 3, 5, 2, 6, 1, 7):
        send(("merge z", k), mzbuf.at[e], mzbuf.at[e], device("z", k))
    for k in (1, 7, 2, 6, 3, 5, 4):
        wait(("merge z", k), mzbuf.at[at("z", -k)])
    top, whole = merge([(mzbuf[k, 0:1, :], mzbuf[k, 1:2, :]) for k in range(NZ)])
    mybuf[m, 0:1, :] = top
    mybuf[m, 1:2, :] = whole
    for k in (2, 1, 3):
        send(("merge y", k), mybuf.at[m], mybuf.at[m], device("y", k))
    for k in (1, 3, 2):
        wait(("merge y", k), mybuf.at[at("y", -k)])
    top, whole = merge([(mybuf[k, 0:1, :], mybuf[k, 1:2, :]) for k in range(NY)])
    head_logsum = top + jnp.log(whole)
    lse_ref[...] = head_logsum

    def spread(row):
        return jnp.broadcast_to(jnp.sum(row * row, axis=1, keepdims=True), (1, LANE))

    pbuf[d, 0:1, :] = spread(router_logsum)
    pbuf[d, 1:2, :] = spread(head_logsum)
    for k in range(NX):
        send(("penalty", 1, k), pbuf.at[d], pbuf.at[d], core(k))
        if k > 0:
            send(("penalty", 0, k), pbuf.at[d], pbuf.at[d], device("x", k))
    for k in range(NX):
        wait(("penalty", 1, k), pbuf.at[at("x", -k) * 2 + (1 - c)])
        if k > 0:
            wait(("penalty", 0, k), pbuf.at[at("x", -k) * 2 + c])
    sums = pbuf[0, 0:2, :]
    for k in range(1, 2 * NX):
        sums = sums + pbuf[k, 0:2, :]
    rp_ref[...] = sums[0:1, :] / (2 * NX * TOK)
    hp_ref[...] = sums[1:2, :] / (2 * NX * TOK)

    for copy in sent:
        copy.wait_send()


def body(tokens, expert_index, slot_index, norm_gain, router_weight, gate_weight, up_weight,
         down_weight, final_gain, head_weight):
    vmem = pl.BlockSpec(memory_space=pltpu.VMEM)
    hbm = pl.BlockSpec(memory_space=pl.ANY)
    scratch = [
        pltpu.VMEM((HID2, WIDTH), BF16),
        pltpu.VMEM((HID2, WIDTH), BF16),
        pltpu.VMEM((HID2, WIDTH), BF16),
        pltpu.VMEM((512, WIDTH), BF16),
        pltpu.VMEM((NZ, CAP, LANE), BF16),
        pltpu.VMEM((NY, NX, NZ, CAP, LANE), BF16),
        pltpu.VMEM((ROWS, HID2), F32),
        pltpu.VMEM((ROWS, HID2), F32),
        pltpu.VMEM((ROWS, HID2), BF16),
        pltpu.VMEM((NY, NX, NZ, CAP, LANE), BF16),
        pltpu.VMEM((4, 2, 2, CAP, LANE), BF16),
        pltpu.VMEM((4, 2, 4, CAP, LANE), BF16),
        pltpu.VMEM((4, 2, 2, CAP, LANE), BF16),
        pltpu.VMEM((4, 2, 4, CAP, LANE), BF16),
        pltpu.VMEM((4, 4, CAP, LANE), BF16),
        pltpu.VMEM((4, 4, CAP, LANE), BF16),
        pltpu.VMEM((2, 2, CAP, LANE), BF16),
        pltpu.VMEM((2, 4, CAP, LANE), BF16),
        pltpu.VMEM((2, 2, CAP, LANE), BF16),
        pltpu.VMEM((2, 4, CAP, LANE), BF16),
        pltpu.VMEM((NZ, CAP, LANE), BF16),
        pltpu.VMEM((NZ, CAP, LANE), BF16),
        pltpu.VMEM((TOK, NZ * CAP), BF16),
        pltpu.VMEM((TOK, NZ * CAP), BF16),
        pltpu.VMEM((NY, NZ, TOK, LANE), BF16),
        pltpu.VMEM((520, TOK), F32),
        pltpu.VMEM((NZ, 16, TOK), F32),
        pltpu.VMEM((NY, 16, TOK), F32),
        pltpu.VMEM((NX, 8, LANE), F32),
        pltpu.VMEM((NZ, 8, TOK), F32),
        pltpu.VMEM((NY, 8, TOK), F32),
        pltpu.VMEM((2 * NX, 8, LANE), F32),
        pltpu.SemaphoreType.DMA((SEMS,)),
        pltpu.SemaphoreType.DMA((SEMS,)),
        pltpu.SemaphoreType.DMA((4,)),
    ]
    layer_out, head_logsum, router_penalty, head_penalty = pl.pallas_call(
        kernel,
        name="layer",
        out_shape=(
            jax.ShapeDtypeStruct((TOK, LANE), BF16),
            jax.ShapeDtypeStruct((1, TOK), F32),
            jax.ShapeDtypeStruct((1, LANE), F32),
            jax.ShapeDtypeStruct((1, LANE), F32),
        ),
        in_specs=[vmem] * 6 + [hbm] * 4,
        out_specs=(vmem,) * 4,
        scratch_shapes=scratch,
        compiler_params=pltpu.CompilerParams(
            collective_id=0, has_side_effects=True, vmem_limit_bytes=56 * 1024 * 1024
        ),
    )(
        tokens, expert_index.T, slot_index.T, norm_gain[None, :], router_weight,
        final_gain[None, :], gate_weight[0], up_weight[0], down_weight[0], head_weight,
    )
    return layer_out, head_logsum[0], router_penalty[0, 0], head_penalty[0, 0]


def solution(mesh):
    in_specs = (
        P("dp", ("expert", "mp")),
        P("dp", None),
        P("dp", None),
        P(("expert", "mp")),
        P(None, ("expert", "mp")),
        P("expert", ("dp", "mp"), None),
        P("expert", ("dp", "mp"), None),
        P("expert", ("dp", "mp"), None),
        P(),
        P(("expert", "mp"), None),
    )
    out_specs = (P("dp", ("expert", "mp")), P("dp"), P(), P())
    return jax.shard_map(body, mesh=mesh, in_specs=in_specs, out_specs=out_specs, check_vma=False)
```

```python
import jax
import jax.numpy as jnp
from jax import lax
from jax.experimental import pallas as pl
from jax.experimental.pallas import tpu as pltpu
from jax.sharding import PartitionSpec as P

F32 = jnp.float32
BF16 = jnp.bfloat16
EPSILON = 1e-05
LAST = (((1,), (1,)), ((), ()))
EXACT = lax.Precision.HIGHEST

NX, NY, NZ = 4, 4, 8
CAP = 96
TOK = 256
LANE = 128
HID = 224
HID2 = 2 * HID
WIDTH = LANE * NY * NZ
ROWS = NX * CAP
SENDS = 64
ARRIVALS = 115
CUT_A, CUT_B = 192, 256
SUB_A, SUB_B = 96, 224


def kernel(
    tk_h, ei_h, si_h, ng_h, rw_h, fg_h, gw_h, uw_h, dw_h, hw_h,
    out_ref, lse_ref, rp_ref, hp_ref,
    tk, ei, si, ng, rw, fg,
    w3, hw, ls, xs, acc_g, acc_u, hid, ps, ra_a, rb_a, ra_b, rb_b, sa, sb,
    ra2_a, rb2_a, ra2_b, rb2_b, fin, rx, chi, clo, hs, acc_h,
    zbuf, ybuf, ibuf, mzbuf, mybuf, ssem, rsem, lsem,
):
    d = lax.axis_index("dp")
    e = lax.axis_index("expert")
    m = lax.axis_index("mp")
    x = d // 2
    c = d % 2
    gw, uw, dw = w3.at[0], w3.at[1], w3.at[2]
    coord = {"x": x, "y": m, "z": e}
    size = {"x": NX, "y": NY, "z": NZ}

    def at(axis, step):
        return (coord[axis] + step + size[axis]) % size[axis]

    def device(axis, step):
        if axis == "x":
            return {"dp": at("x", step) * 2 + c, "expert": e, "mp": m}
        if axis == "y":
            return {"dp": d, "expert": e, "mp": at("y", step)}
        return {"dp": d, "expert": at("z", step), "mp": m}

    def plane(step_x, step_y, other):
        dp = at("x", step_x) * 2 + (1 - c if other else c)
        return {"dp": dp, "expert": e, "mp": at("y", step_y)}

    ids = {}
    sent = []
    scopes = []

    def phase(name):
        while scopes:
            scopes.pop().__exit__(None, None, None)
        if name:
            scopes.append(jax.named_scope(name))
            scopes[-1].__enter__()


    def remote(tag, slot, src, dst, dev):
        number = ids.setdefault(tag, len(ids))
        return pltpu.make_async_remote_copy(
            src_ref=src, dst_ref=dst, send_sem=ssem.at[slot], recv_sem=rsem.at[number],
            device_id=dev, device_id_type=pl.DeviceIdType.MESH,
        )

    def send(tag, src, dst, dev):
        if len(sent) >= SENDS:
            sent[-SENDS].wait_send()
        copy = remote(tag, len(sent) % SENDS, src, dst, dev)
        copy.start()
        sent.append(copy)

    def wait(tag, ref):
        remote(tag, 0, ref, ref, device("y", 1)).wait_recv()

    phase("entry")
    smalls = [
        pltpu.make_async_copy(source, held, lsem.at[4 + number])
        for number, (source, held) in enumerate(
            ((tk_h, tk), (ei_h, ei), (si_h, si), (ng_h, ng), (rw_h, rw), (fg_h, fg))
        )
    ]
    loads = [
        pltpu.make_async_copy(gw_h, gw.at[pl.ds(0, HID)], lsem.at[0]),
        pltpu.make_async_copy(uw_h, uw.at[pl.ds(0, HID)], lsem.at[1]),
        pltpu.make_async_copy(dw_h, dw.at[pl.ds(0, HID)], lsem.at[2]),
        pltpu.make_async_copy(hw_h, hw, lsem.at[3]),
    ]
    barrier = pltpu.get_barrier_semaphore()
    partners = [device("z", k) for k in range(1, NZ)]
    others = [
        (step_x, step_y, other)
        for step_x in (2, 1, 3, 0) for step_y in (2, 1, 3, 0) for other in (True, False)
        if (step_x, step_y, other) != (0, 0, False)
    ]
    partners += [plane(*step) for step in others]
    for partner in partners:
        pl.semaphore_signal(
            barrier, inc=1, device_id=partner, device_id_type=pl.DeviceIdType.MESH
        )

    phase("choose")
    for load in smalls + loads:
        load.start()
    for load in smalls:
        load.wait()

    t32 = tk[...].astype(F32)
    gained = (t32 * ng[...]).astype(BF16)
    flat0 = ei[0:1, :] * CAP + si[0:1, :]
    flat1 = ei[1:2, :] * CAP + si[1:2, :]
    slot_iota = lax.broadcasted_iota(jnp.int32, (CAP, TOK), 0)
    for ex in range(NZ):
        rows = slot_iota + ex * CAP
        choose = jnp.where((rows == flat0) | (rows == flat1), 1.0, 0.0).astype(BF16)
        ls[ex] = jnp.dot(choose, gained, preferred_element_type=F32).astype(BF16)
    router_gained = rw[...].astype(F32) * ng[...]
    zbuf[e, 0:8, :] = lax.dot_general(
        router_gained, t32, LAST, precision=EXACT, preferred_element_type=F32
    )
    ones8 = jnp.ones((8, LANE), F32)
    zbuf[e, 8:16, :] = lax.dot_general(
        ones8, t32 * t32, LAST, precision=EXACT, preferred_element_type=F32
    )
    xs[m, x, 0] = ls[e]

    phase("barrier")
    pl.semaphore_wait(barrier, len(partners))
    for k in (4, 3, 5, 2, 6, 1, 7):
        send("slots", ls.at[at("z", k)], xs.at[m, x, NZ - k], device("z", k))
    for k in range(1, NZ):
        send("router z", zbuf.at[e], zbuf.at[e], device("z", k))
    for load in loads:
        load.wait()
    send("weights", w3.at[:, pl.ds(0, HID)], w3.at[:, pl.ds(HID, HID)], plane(0, 0, True))

    phase("slots_wait")
    def ring(rounds, start, tag, axis, view):
        def begin():
            send((tag, "+", 1), view(coord[axis]), view(coord[axis]), device(axis, 1))
            send((tag, "-", 1), view(coord[axis]), view(coord[axis]), device(axis, -1))

        def step():
            for sign, toward, part in (("+", 1, 0), ("-", -1, 1)):
                source = at(axis, -toward)
                wait((tag, sign, 1), view(source))
                unit = view(source, part)
                send((tag, 2), unit, unit, device(axis, toward))

        def finish():
            wait((tag, 2), view(at(axis, 2)))

        for number, event in enumerate((begin, step, finish)):
            rounds.setdefault(start + number, []).append(event)

    def play(rounds, number):
        for event in rounds.get(number, []):
            event()

    def slab(yy, xx, first):
        def view(part=None):
            if part is None:
                return xs.at[yy, xx, pl.ds(first, 4)]
            return xs.at[yy, xx, pl.ds(first + 2 * part, 2)]
        return view

    gather = {}
    ring(gather, 0, "ga x", "x", lambda s, p=None: slab(m, s, 0)(p))
    ring(gather, 0, "gb y", "y", lambda s, p=None: slab(s, x, 4)(p))
    for step_, start in ((2, 2), (1, 1), (-1, 1), (0, 0)):
        ring(gather, start, ("ga y", step_), "y",
             lambda s, p=None, t=step_: slab(s, at("x", t), 0)(p))
        ring(gather, start, ("gb x", step_), "x",
             lambda s, p=None, t=step_: slab(at("y", t), s, 4)(p))

    wait("slots", xs.at[m, x, pl.ds(1, NZ - 1)])
    play(gather, 0)

    phase("router_z")
    wait("router z", zbuf.at[pl.ds(0, NZ - 1)])
    total = zbuf[0]
    for k in range(1, NZ):
        total = total + zbuf[k]
    ybuf[m] = total
    for k in range(1, NY):
        send("router y", ybuf.at[m], ybuf.at[m], device("y", k))

    phase("gain")
    @pl.loop(0, 512 // 16)
    def _(i):
        part = pl.ds(pl.multiple_of(i * 16, 16), 16)
        hw[part, :] = (hw[part, :].astype(F32) * fg[...]).astype(BF16)

    phase("gather1")
    play(gather, 1)

    phase("router_y")
    wait("router y", ybuf.at[pl.ds(0, NY - 1)])
    total = ((ybuf[0] + ybuf[1]) + ybuf[2]) + ybuf[3]
    inverse8 = lax.rsqrt(total[8:16] / WIDTH + EPSILON)
    logits = total[0:8] * inverse8
    expert_iota = lax.broadcasted_iota(jnp.int32, (8, TOK), 0)
    place = slot_iota + e * CAP
    mine = jnp.where((place == flat0) | (place == flat1), 1.0, 0.0)
    mine = jnp.concatenate([mine, jnp.zeros((LANE - CAP, TOK), F32)], axis=0)
    ibuf[x] = lax.dot_general(
        inverse8, mine, LAST, precision=EXACT, preferred_element_type=F32
    )
    for k in range(1, NX):
        send("inverse", ibuf.at[x], ibuf.at[x], device("x", k))

    phase("gather2")
    play(gather, 2)

    phase("router_c")
    top = jnp.max(logits, axis=0, keepdims=True)
    router_logsum = top + jnp.log(jnp.sum(jnp.exp(logits - top), axis=0, keepdims=True))
    picked0 = jnp.sum(jnp.where(expert_iota == ei[0:1, :], logits, 0.0), axis=0, keepdims=True)
    picked1 = jnp.sum(jnp.where(expert_iota == ei[1:2, :], logits, 0.0), axis=0, keepdims=True)
    higher = jnp.maximum(picked0, picked1)
    power0 = jnp.exp(picked0 - higher)
    power1 = jnp.exp(picked1 - higher)
    weight0 = power0 / (power0 + power1)
    weight1 = power1 / (power0 + power1)
    chunk_iota = lax.broadcasted_iota(jnp.int32, (LANE, TOK), 0)
    for j in range(NZ * CAP // LANE):
        rows = chunk_iota + j * LANE
        mixed = jnp.where(rows == flat0, weight0, 0.0) + jnp.where(rows == flat1, weight1, 0.0)
        mixed = mixed.T
        high = mixed.astype(BF16)
        chi[:, j * LANE:(j + 1) * LANE] = high
        clo[:, j * LANE:(j + 1) * LANE] = (mixed - high.astype(F32)).astype(BF16)
    acc_g[...] = jnp.zeros_like(acc_g)
    acc_u[...] = jnp.zeros_like(acc_u)

    phase("gather3")
    play(gather, 3)
    wait("weights", w3.at[:, pl.ds(HID, HID)])
    wait("inverse", ibuf.at[pl.ds(0, NX - 1)])
    phase("gather4")
    play(gather, 4)

    phase("gateup")
    def columns(weight, ex, yy):
        block = (ex % NZ) * NY + yy
        return weight[:, pl.ds(pl.multiple_of(block * LANE, LANE), LANE)]

    @pl.loop(0, NY)
    def _(yy):
        held = jnp.concatenate(
            [xs[yy, :, j].reshape(ROWS, LANE) for j in range(NZ)], axis=1
        )
        for acc, weight in ((acc_g, gw), (acc_u, uw)):
            against = jnp.concatenate([columns(weight, e + j, yy) for j in range(NZ)], axis=1)
            acc[...] += lax.dot_general(held, against, LAST, preferred_element_type=F32)

    for xx in range(NX):
        rows = pl.ds(xx * CAP, CAP)
        scale = jnp.broadcast_to(ibuf[xx, 0:1, :], (LANE, LANE)).T[0:CAP, 0:1]
        gate_value = acc_g[rows, :] * scale
        up_value = acc_u[rows, :] * scale
        hid[rows, :] = (gate_value / (1.0 + jnp.exp(-gate_value)) * up_value).astype(BF16)

    phase("down")
    def down(yy, first):
        against = jnp.concatenate([columns(dw, e + first + j, yy) for j in range(4)], axis=1)
        product = jnp.dot(hid[...], against, preferred_element_type=F32).astype(BF16)
        for j in range(4):
            for xx in range(NX):
                ps[yy, xx, first + j] = product[
                    xx * CAP:(xx + 1) * CAP, j * LANE:(j + 1) * LANE
                ]

    def reduce_first(tag, axis, view, near):
        send((tag, "+", 1), view(at(axis, 2), 0), near.at[0], device(axis, 1))
        send((tag, "-", 1), view(at(axis, 2), 1), near.at[1], device(axis, -1))

    def add_into(target, source):
        target[...] = (target[...].astype(F32) + source[...].astype(F32)).astype(BF16)

    def reduce_second(tag, axis, view, near, far):
        wait((tag, "+", 1), near.at[0])
        add_into(view(at(axis, 1), 0), near.at[0])
        send((tag, 2), view(at(axis, 1)), far.at[0], device(axis, 1))
        wait((tag, "-", 1), near.at[1])
        add_into(view(at(axis, -1), 1), near.at[1])
        send((tag, 2), view(at(axis, -1)), far.at[1], device(axis, -1))

    def reduce_last(tag, view, far, into):
        wait((tag, 2), far)
        into[...] = (
            view[...].astype(F32) + far[0].astype(F32) + far[1].astype(F32)
        ).astype(BF16)

    def part_a(yy, xx, part=None):
        if part is None:
            return ps.at[yy, xx, pl.ds(0, 4)]
        return ps.at[yy, xx, pl.ds(2 * part, 2)]

    def part_b(yy, xx, part=None):
        if part is None:
            return ps.at[yy, xx, pl.ds(4, 4)]
        return ps.at[yy, xx, pl.ds(4 + 2 * part, 2)]

    order = (2, 1, -1, 0)

    def a_view(t):
        return lambda s, p=None: part_a(s, at("x", t), p)

    def b_view(t):
        return lambda s, p=None: part_b(at("y", t), s, p)

    down(at("y", 2), 0)
    for i, t in enumerate(order):
        reduce_first(("ra y", t), "y", a_view(t), ra_a.at[i])

    @pl.loop(0, NY)
    def _(k):
        down((m + 2 + k) % NY, 4)

    for i, t in enumerate(order):
        reduce_first(("rb x", t), "x", b_view(t), ra_b.at[i])

    @pl.loop(1, NY)
    def _(k):
        down((m + 2 + k) % NY, 0)

    phase("reduce2")
    for i, t in enumerate(order):
        reduce_second(("ra y", t), "y", a_view(t), ra_a.at[i], rb_a.at[i])
        reduce_second(("rb x", t), "x", b_view(t), ra_b.at[i], rb_b.at[i])

    def sa_view(s, p=None):
        return sa.at[s] if p is None else sa.at[s, pl.ds(2 * p, 2)]

    def sb_view(s, p=None):
        return sb.at[s] if p is None else sb.at[s, pl.ds(2 * p, 2)]

    phase("reduce3")
    for i, t in enumerate(order):
        reduce_last(("ra y", t), a_view(t)(m), rb_a.at[i], sa.at[at("x", t)])
        if t == 2:
            reduce_first("ra x", "x", sa_view, ra2_a)
        reduce_last(("rb x", t), b_view(t)(x), rb_b.at[i], sb.at[at("y", t)])
        if t == 2:
            reduce_first("rb y", "y", sb_view, ra2_b)
        if t == -1:
            reduce_second("ra x", "x", sa_view, ra2_a, rb2_a)
            reduce_second("rb y", "y", sb_view, ra2_b, rb2_b)
    reduce_last("ra x", sa_view(x), rb2_a, fin.at[pl.ds(0, 4)])
    reduce_last("rb y", sb_view(m), rb2_b, fin.at[pl.ds(4, 4)])

    phase("back")
    for k in (4, 3, 5, 2, 6, 1, 7):
        send("back", fin.at[k], rx.at[e], device("z", k))
    rx[e] = fin[0]
    wait("back", rx.at[pl.ds(0, NZ - 1)])
    phase("combine")
    outputs = rx[...].reshape(NZ * CAP, LANE)
    combined = jnp.dot(chi[...], outputs, preferred_element_type=F32)
    combined += jnp.dot(clo[...], outputs, preferred_element_type=F32)
    layer_out = (tk[...].astype(F32) + combined).astype(BF16)
    out_ref[...] = layer_out
    hs[m, e] = layer_out

    phase("head_gather")
    def rows_a(yy, zz, part=None):
        if part is None:
            return hs.at[yy, zz, pl.ds(0, CUT_A)]
        return hs.at[yy, zz, pl.ds(0, SUB_A)] if part == 0 else hs.at[
            yy, zz, pl.ds(SUB_A, CUT_A - SUB_A)]

    def rows_b(yy, zz, part=None):
        if part is None:
            return hs.at[yy, zz, pl.ds(CUT_A, CUT_B - CUT_A)]
        return hs.at[yy, zz, pl.ds(CUT_A, SUB_B - CUT_A)] if part == 0 else hs.at[
            yy, zz, pl.ds(SUB_B, CUT_B - SUB_B)]

    def ring8(rounds, start, tag, view, times):
        def begin():
            for k in (2, 1):
                for sign, toward in (("+", 1), ("-", -1)):
                    send((tag, sign, 2) if k == 2 else (tag, 1), view(e), view(e), device("z", toward * k))

        def step():
            for sign, toward, part in (("+", 1, 0), ("-", -1, 1)):
                source = at("z", -toward * 2)
                wait((tag, sign, 2), view(source))
                unit = view(source, part)
                send((tag, 3), unit, unit, device("z", toward * 2))
                send((tag, 3), view(source), view(source), device("z", toward))
            wait((tag, 1), times(2))

        def finish():
            wait((tag, 3), times(3))

        for number, event in enumerate((begin, step, finish)):
            rounds.setdefault(start + number, []).append(event)

    def logits_chunk(yy):
        held = jnp.concatenate([hs[yy, zz] for zz in range(NZ)], axis=1)
        against = jnp.concatenate([columns(hw, zz, yy) for zz in range(NZ)], axis=1)
        acc_h[0:512, :] += lax.dot_general(against, held, LAST, preferred_element_type=F32)
        squares = jnp.zeros((TOK, LANE), F32)
        for zz in range(NZ):
            block = hs[yy, zz].astype(F32)
            squares = squares + block * block
        acc_h[512:520, :] += lax.dot_general(
            ones8, squares, LAST, precision=EXACT, preferred_element_type=F32
        )

    head = {}
    ring(head, 0, "hb y", "y", lambda s, p=None: rows_b(s, e, p))
    ring8(head, 0, "ha z", lambda s, p=None: rows_a(m, s, p),
          lambda n: hs.at[m, pl.ds(0, n), pl.ds(0, CUT_A)])
    for start, near, far in ((2, (3, -3, 4), (2,)), (1, (1, -1, 2, -2), (1, -1)), (0, (0,), (0,))):
        for t in far:
            ring8(head, start, ("hb z", t), lambda s, p=None, t=t: rows_b(at("y", t), s, p),
                  lambda n, t=t: hs.at[at("y", t), pl.ds(0, n), pl.ds(CUT_A, CUT_B - CUT_A)])
        for t in near:
            ring(head, start, ("ha y", t), "y", lambda s, p=None, t=t: rows_a(s, at("z", t), p))
    play(head, 0)
    acc_h[...] = jnp.zeros_like(acc_h)
    play(head, 1)
    play(head, 2)

    logits_chunk(m)
    play(head, 3)
    phase("logits")

    @pl.loop(0, 2)
    def _(k):
        logits_chunk((m + 1 + 2 * k) % NY)

    play(head, 4)
    phase("logits2")
    logits_chunk(at("y", 2))

    head_scale = lax.rsqrt(acc_h[512:513, :] / WIDTH + EPSILON)
    vocab = acc_h[0:512, :] * head_scale

    def logsum(rows):
        top = jnp.max(rows, axis=0, keepdims=True)
        return top + jnp.log(jnp.sum(jnp.exp(rows - top), axis=0, keepdims=True))

    def merged(rows):
        top = rows[0]
        for row in rows[1:]:
            top = jnp.maximum(top, row)
        whole = jnp.exp(rows[0] - top)
        for row in rows[1:]:
            whole = whole + jnp.exp(row - top)
        return top + jnp.log(whole)

    mzbuf[e] = logsum(vocab)
    phase("merge_z")
    for k in (4, 3, 5, 2, 6, 1, 7):
        send("merge z", mzbuf.at[e], mzbuf.at[e], device("z", k))
    wait("merge z", mzbuf.at[pl.ds(0, NZ - 1)])
    mybuf[d * NY + m, 0:1, :] = merged([mzbuf[k] for k in range(NZ)])
    mybuf[d * NY + m, 1:2, :] = router_logsum
    phase("merge_xy")
    for step in others:
        send("merge xy", mybuf.at[d * NY + m], mybuf.at[d * NY + m], plane(*step))
    wait("merge xy", mybuf.at[pl.ds(0, len(others))])
    phase("penalty")
    router_sum = jnp.zeros((1, TOK), F32)
    head_sum = jnp.zeros((1, TOK), F32)
    for dp in range(2 * NX):
        routed = mybuf[dp * NY, 1:2, :]
        router_sum = router_sum + routed * routed
        ended = merged([mybuf[dp * NY + yy, 0:1, :] for yy in range(NY)])
        head_sum = head_sum + ended * ended
    lse_ref[...] = merged([mybuf[d * NY + yy, 0:1, :] for yy in range(NY)])

    def spread(row):
        return jnp.broadcast_to(jnp.sum(row, axis=1, keepdims=True), (1, LANE))

    rp_ref[...] = spread(router_sum) / (2 * NX * TOK)
    hp_ref[...] = spread(head_sum) / (2 * NX * TOK)

    phase("drain")
    for copy in sent[-SENDS:]:
        copy.wait_send()
    phase("")
    assert len(ids) == ARRIVALS


def body(tokens, expert_index, slot_index, norm_gain, router_weight, gate_weight, up_weight,
         down_weight, final_gain, head_weight):
    vmem = pl.BlockSpec(memory_space=pltpu.VMEM)
    hbm = pl.BlockSpec(memory_space=pl.ANY)
    scratch = [
        pltpu.VMEM((TOK, LANE), BF16),
        pltpu.VMEM((2, TOK), jnp.int32),
        pltpu.VMEM((2, TOK), jnp.int32),
        pltpu.VMEM((1, LANE), F32),
        pltpu.VMEM((8, LANE), BF16),
        pltpu.VMEM((1, WIDTH), F32),
        pltpu.VMEM((3, HID2, WIDTH), BF16),
        pltpu.VMEM((512, WIDTH), BF16),
        pltpu.VMEM((NZ, CAP, LANE), BF16),
        pltpu.VMEM((NY, NX, NZ, CAP, LANE), BF16),
        pltpu.VMEM((ROWS, HID2), F32),
        pltpu.VMEM((ROWS, HID2), F32),
        pltpu.VMEM((ROWS, HID2), BF16),
        pltpu.VMEM((NY, NX, NZ, CAP, LANE), BF16),
        pltpu.VMEM((4, 2, 2, CAP, LANE), BF16),
        pltpu.VMEM((4, 2, 4, CAP, LANE), BF16),
        pltpu.VMEM((4, 2, 2, CAP, LANE), BF16),
        pltpu.VMEM((4, 2, 4, CAP, LANE), BF16),
        pltpu.VMEM((4, 4, CAP, LANE), BF16),
        pltpu.VMEM((4, 4, CAP, LANE), BF16),
        pltpu.VMEM((2, 2, CAP, LANE), BF16),
        pltpu.VMEM((2, 4, CAP, LANE), BF16),
        pltpu.VMEM((2, 2, CAP, LANE), BF16),
        pltpu.VMEM((2, 4, CAP, LANE), BF16),
        pltpu.VMEM((NZ, CAP, LANE), BF16),
        pltpu.VMEM((NZ, CAP, LANE), BF16),
        pltpu.VMEM((TOK, NZ * CAP), BF16),
        pltpu.VMEM((TOK, NZ * CAP), BF16),
        pltpu.VMEM((NY, NZ, TOK, LANE), BF16),
        pltpu.VMEM((520, TOK), F32),
        pltpu.VMEM((NZ, 16, TOK), F32),
        pltpu.VMEM((NY, 16, TOK), F32),
        pltpu.VMEM((NX, 8, LANE), F32),
        pltpu.VMEM((NZ, 1, TOK), F32),
        pltpu.VMEM((2 * NX * NY, 2, TOK), F32),
        pltpu.SemaphoreType.DMA((SENDS,)),
        pltpu.SemaphoreType.DMA((ARRIVALS,)),
        pltpu.SemaphoreType.DMA((10,)),
    ]
    layer_out, head_logsum, router_penalty, head_penalty = pl.pallas_call(
        kernel,
        name="layer",
        out_shape=(
            jax.ShapeDtypeStruct((TOK, LANE), BF16),
            jax.ShapeDtypeStruct((1, TOK), F32),
            jax.ShapeDtypeStruct((1, LANE), F32),
            jax.ShapeDtypeStruct((1, LANE), F32),
        ),
        in_specs=[hbm] * 10,
        out_specs=(vmem,) * 4,
        scratch_shapes=scratch,
        compiler_params=pltpu.CompilerParams(
            collective_id=0, has_side_effects=True, vmem_limit_bytes=56 * 1024 * 1024
        ),
    )(
        tokens, expert_index.T, slot_index.T, norm_gain[None, :], router_weight,
        final_gain[None, :], gate_weight[0], up_weight[0], down_weight[0], head_weight,
    )
    return layer_out, head_logsum[0], router_penalty[0, 0], head_penalty[0, 0]


def solution(mesh):
    in_specs = (
        P("dp", ("expert", "mp")),
        P("dp", None),
        P("dp", None),
        P(("expert", "mp")),
        P(None, ("expert", "mp")),
        P("expert", ("dp", "mp"), None),
        P("expert", ("dp", "mp"), None),
        P("expert", ("dp", "mp"), None),
        P(),
        P(("expert", "mp"), None),
    )
    out_specs = (P("dp", ("expert", "mp")), P("dp"), P(), P())
    return jax.shard_map(body, mesh=mesh, in_specs=in_specs, out_specs=out_specs, check_vma=False)
```

```python
import jax
import jax.numpy as jnp
from jax import lax
from jax.experimental import pallas as pl
from jax.experimental.pallas import tpu as pltpu
from jax.sharding import PartitionSpec as P

F32 = jnp.float32
BF16 = jnp.bfloat16
EPSILON = 1e-05
LAST = (((1,), (1,)), ((), ()))
EXACT = lax.Precision.HIGHEST

NX, NY, NZ = 4, 4, 8
CAP = 96
TOK = 256
LANE = 128
HID = 224
HID2 = 2 * HID
WIDTH = LANE * NY * NZ
ROWS = NX * CAP
SENDS = 64
ARRIVALS = 168
CUT_A, CUT_B = 192, 256
SUB_A, SUB_B = 96, 224


class Plan:
    RATE, FIRST, HOP = 46.6e3, 2.6, 0.75

    def __init__(self):
        self.sends, self.works, self.waits, self.given = [], [], {}, {}

    def send(self, group, link, size, needs, emit, hops=1):
        self.sends.append([group, link, size / self.RATE, frozenset(needs), emit, hops])

    def send_both(self, group, axis, size, needs, emit, hops):
        self.send(group, axis + "+", size / 2, needs, emit, hops)
        self.send(group, axis + "-", size / 2, needs, lambda: None, hops)

    def wait(self, group, emit):
        self.waits[group] = emit

    def arrives(self, group, needs, delay, emit):
        self.given[group] = (frozenset(needs), delay)
        self.waits[group] = emit

    def work(self, name, time, needs, emit):
        self.works.append([name, time, frozenset(needs), emit])

    def chains(self):
        after = {}
        for group, _, time, needs, _, hops in self.sends:
            for need in needs:
                after.setdefault(need, []).append(
                    (time + self.FIRST + self.HOP * (hops - 1), group))
        for name, time, needs, _ in self.works:
            for need in needs:
                after.setdefault(need, []).append((time, name))
        for group, (needs, delay) in self.given.items():
            for need in needs:
                after.setdefault(need, []).append((delay, group))
        memo = {}

        def rest(event):
            if event not in memo:
                memo[event] = max((t + rest(n) for t, n in after.get(event, [])), default=0.0)
            return memo[event]

        return rest

    def run(self):
        horizons = (0.3, 0.5, 0.7, 1.0, 1.5)
        return self.play(min(horizons, key=lambda h: self.play(h, False)))

    def play(self, horizon, real=True):
        rest = self.chains()
        clock, free, had = 0.0, {}, set()
        sends, works = list(self.sends), list(self.works)
        left, when, due, done = {}, {}, {}, set()
        for item in sends:
            left[item[0]] = left.get(item[0], 0) + 1

        def issue(force):
            nonlocal sends
            ready = [item for item in sends if item[3] <= had]
            ready.sort(key=lambda item: -(item[2] + rest(item[0])))
            gone = []
            for item in ready:
                group, link, time, _, emit, hops = item
                if free.get(link, 0.0) > clock + horizon and not force:
                    continue
                if real:
                    emit()
                free[link] = max(clock, free.get(link, 0.0)) + time * hops
                arrival = free[link] + self.FIRST + self.HOP * (hops - 1)
                when[group] = max(when.get(group, 0.0), arrival)
                left[group] -= 1
                if left[group] == 0:
                    due[group] = when[group]
                gone.append(id(item))
            sends = [item for item in sends if id(item) not in gone]

        while True:
            for group, (needs, delay) in self.given.items():
                if group not in due and needs <= had:
                    due[group] = clock + delay
            issue(False)
            coming = sorted((time, str(group), group) for group, time in due.items()
                            if group not in done)
            ready = [item for item in works if item[2] <= had]
            ready.sort(key=lambda item: -(item[1] + rest(item[0])))
            chosen = None
            for item in ready:
                if not coming or coming[0][0] - clock >= 0.6 * item[1] or (
                        rest(item[0]) + item[1] > rest(coming[0][2]) + 1.0):
                    chosen = item
                    break
            if chosen is not None:
                works = [item for item in works if item is not chosen]
                if real:
                    chosen[3]()
                clock += chosen[1]
                had.add(chosen[0])
            elif coming:
                time, _, group = coming[0]
                if real:
                    self.waits[group]()
                clock = max(clock, time) + 0.01
                done.add(group)
                had.add(group)
            elif sends:
                issue(True)
            else:
                break
        return clock


def kernel(
    tk_h, ei_h, si_h, ng_h, rw_h, fg_h, gw_h, uw_h, dw_h, hw_h,
    out_ref, lse_ref, rp_ref, hp_ref,
    tk, ei, si, ng, rw, fg,
    w3, hw, ls, xs, acc_g, acc_u, hid, ps, near1, far1,
    sums, near2, far2, fin, rx, chi, clo, hs, acc_h, squares,
    zbuf, ybuf, rbuf, ibuf, mzbuf, mybuf, ssem, rsem, lsem,
):
    d = lax.axis_index("dp")
    e = lax.axis_index("expert")
    m = lax.axis_index("mp")
    x = d // 2
    c = d % 2
    gw, uw, dw = w3.at[0], w3.at[1], w3.at[2]
    coord = {"x": x, "y": m, "z": e}
    extent = {"x": NX, "y": NY, "z": NZ}

    def at(axis, step):
        return (coord[axis] + step + extent[axis]) % extent[axis]

    def device(axis, step):
        if axis == "x":
            return {"dp": at("x", step) * 2 + c, "expert": e, "mp": m}
        if axis == "y":
            return {"dp": d, "expert": e, "mp": at("y", step)}
        return {"dp": d, "expert": at("z", step), "mp": m}

    def plane(step_x, step_y, other):
        dp = at("x", step_x) * 2 + (1 - c if other else c)
        return {"dp": dp, "expert": e, "mp": at("y", step_y)}

    ids = {}
    sent = []
    scopes = []

    def phase(name):
        while scopes:
            scopes.pop().__exit__(None, None, None)
        if name:
            scopes.append(jax.named_scope(name))
            scopes[-1].__enter__()


    def remote(tag, slot, src, dst, dev):
        number = ids.setdefault(tag, len(ids))
        return pltpu.make_async_remote_copy(
            src_ref=src, dst_ref=dst, send_sem=ssem.at[slot], recv_sem=rsem.at[number],
            device_id=dev, device_id_type=pl.DeviceIdType.MESH,
        )

    def send(tag, src, dst, dev):
        if len(sent) >= SENDS:
            sent[-SENDS].wait_send()
        copy = remote(tag, len(sent) % SENDS, src, dst, dev)
        copy.start()
        sent.append(copy)

    def wait(tag, ref):
        remote(tag, 0, ref, ref, device("y", 1)).wait_recv()

    phase("entry")
    smalls = [
        pltpu.make_async_copy(source, held, lsem.at[4 + number])
        for number, (source, held) in enumerate(
            ((tk_h, tk), (ei_h, ei), (si_h, si), (ng_h, ng), (rw_h, rw), (fg_h, fg))
        )
    ]
    loads = [
        pltpu.make_async_copy(gw_h, gw.at[pl.ds(0, HID)], lsem.at[0]),
        pltpu.make_async_copy(uw_h, uw.at[pl.ds(0, HID)], lsem.at[1]),
        pltpu.make_async_copy(dw_h, dw.at[pl.ds(0, HID)], lsem.at[2]),
        pltpu.make_async_copy(hw_h, hw, lsem.at[3]),
    ]
    barrier = pltpu.get_barrier_semaphore()
    partners = [device("z", k) for k in range(1, NZ)]
    others = [
        (step_x, step_y, other)
        for step_x in (2, 1, 3, 0) for step_y in (2, 1, 3, 0) for other in (True, False)
        if (step_x, step_y, other) != (0, 0, False)
    ]
    partners += [plane(*step) for step in others]
    for partner in partners:
        pl.semaphore_signal(
            barrier, inc=1, device_id=partner, device_id_type=pl.DeviceIdType.MESH
        )

    phase("choose")
    for load in smalls + loads:
        load.start()
    for load in smalls:
        load.wait()

    t32 = tk[...].astype(F32)
    gained = (t32 * ng[...]).astype(BF16)
    flat0 = ei[0:1, :] * CAP + si[0:1, :]
    flat1 = ei[1:2, :] * CAP + si[1:2, :]
    slot_iota = lax.broadcasted_iota(jnp.int32, (CAP, TOK), 0)
    for ex in range(NZ):
        rows = slot_iota + ex * CAP
        choose = jnp.where((rows == flat0) | (rows == flat1), 1.0, 0.0).astype(BF16)
        ls[ex] = jnp.dot(choose, gained, preferred_element_type=F32).astype(BF16)
    router_gained = rw[...].astype(F32) * ng[...]
    zbuf[e, 0:8, :] = lax.dot_general(
        router_gained, t32, LAST, precision=EXACT, preferred_element_type=F32
    )
    ones8 = jnp.ones((8, LANE), F32)
    zbuf[e, 8:16, :] = lax.dot_general(
        ones8, t32 * t32, LAST, precision=EXACT, preferred_element_type=F32
    )
    xs[m, x, 0] = ls[e]

    phase("barrier")
    pl.semaphore_wait(barrier, len(partners))
    for k in (1, 7, 2, 6, 3, 5, 4):
        send(("slots", min(k, NZ - k)), ls.at[at("z", k)], xs.at[m, x, NZ - k], device("z", k))
    piece = CAP * LANE * 2
    half = CAP // 2

    def slab(yy, xx, j, part=None):
        if part is None:
            return xs.at[yy, xx, j]
        return xs.at[yy, xx, j, pl.ds(half * part, half)]

    plan = Plan()
    phase("gather")

    def ring(plan, tag, axis, size, views, needs, two, one, direct=False):
        if direct:
            for view in views:
                plan.send_both((tag, 2), axis, size, needs, lambda v=view: send(
                    (tag, 2), v(coord[axis]), v(coord[axis]), device(axis, 2)), 2)
        for number, toward in enumerate((1, -1)):
            link = axis + "+-"[number]
            for view in views:
                plan.send((tag, 1), link, size, needs, lambda v=view, w=toward: send(
                    (tag, 1), v(coord[axis]), v(coord[axis]), device(axis, w)))
                if direct:
                    continue
                plan.send((tag, 2), link, size / 2, [(tag, 1)],
                          lambda v=view, w=toward, p=number: send(
                    (tag, 2), v(at(axis, -w), p), v(at(axis, -w), p), device(axis, w)))
        plan.wait((tag, 1), lambda: wait((tag, 1), two))
        plan.wait((tag, 2), lambda: wait((tag, 2), one))

    for k, time in ((1, 3.3), (2, 4.5), (3, 6.0), (4, 7.2)):
        plan.arrives(("slots", k), [], time, lambda k=k: wait(
            ("slots", k), xs.at[m, x, pl.ds(0, 1 if k == 4 else 2)]))
    for j in (0, 7, 1, 6, 2, 5, 3, 4):
        lead, rest = ("x", "y") if j < 4 else ("y", "x")

        def view_of(t, j=j, lead=lead):
            if lead == "x":
                return lambda s, p=None: slab(s, at("x", t), j, p)
            return lambda s, p=None: slab(at("y", t), s, j, p)

        def lead_view(s, p=None, j=j, lead=lead):
            return slab(m, s, j, p) if lead == "x" else slab(s, x, j, p)

        near = [("slots", min(j, NZ - j))] if j > 0 else []
        tag = ("g", j)
        ring(plan, tag, lead, piece, [lead_view], near, xs.at[0, 0, pl.ds(0, 2)], xs.at[0, 0, 0])
        ring(plan, (tag, 0), rest, piece, [view_of(0)], near,
             xs.at[0, 0, pl.ds(0, 2)], xs.at[0, 0, 0])
        ring(plan, (tag, 1), rest, piece, [view_of(1), view_of(-1)], [(tag, 1)],
             xs.at[0, 0, pl.ds(0, 4)], xs.at[0, 0, pl.ds(0, 2)])
        ring(plan, (tag, 2), rest, piece, [view_of(2)], [(tag, 2)],
             xs.at[0, 0, pl.ds(0, 2)], xs.at[0, 0, 0])

    def columns(weight, ex, yy):
        block = (ex % NZ) * NY + yy
        return weight[:, pl.ds(pl.multiple_of(block * LANE, LANE), LANE)]

    def gate_up(yy, first):
        held = jnp.concatenate([xs[yy, :, first + j].reshape(ROWS, LANE) for j in range(4)], axis=1)
        for acc, weight in ((acc_g, gw), (acc_u, uw)):
            against = jnp.concatenate([columns(weight, e + first + j, yy) for j in range(4)], axis=1)
            acc[...] += lax.dot_general(held, against, LAST, preferred_element_type=F32)

    def swap_weights():
        for load in loads:
            load.wait()
        send("weights", w3.at[:, pl.ds(0, HID)], w3.at[:, pl.ds(HID, HID)], plane(0, 0, True))

    def router_start():
        for k in range(1, NZ):
            send("router z", zbuf.at[e], zbuf.at[e], device("z", k))

    def router_middle():
        total = zbuf[0]
        for k in range(1, NZ):
            total = total + zbuf[k]
        ybuf[m] = total
        for k in range(1, NY):
            send("router y", ybuf.at[m], ybuf.at[m], device("y", k))

    def router_end():
        total = ((ybuf[0] + ybuf[1]) + ybuf[2]) + ybuf[3]
        inverse8 = lax.rsqrt(total[8:16] / WIDTH + EPSILON)
        rbuf[...] = total[0:8] * inverse8
        place = slot_iota + e * CAP
        mine = jnp.where((place == flat0) | (place == flat1), 1.0, 0.0)
        mine = jnp.concatenate([mine, jnp.zeros((LANE - CAP, TOK), F32)], axis=0)
        ibuf[x] = lax.dot_general(
            inverse8, mine, LAST, precision=EXACT, preferred_element_type=F32
        )
        for k in range(1, NX):
            send("inverse", ibuf.at[x], ibuf.at[x], device("x", k))

    def gates():
        logits = rbuf[...]
        expert_iota = lax.broadcasted_iota(jnp.int32, (8, TOK), 0)
        top = jnp.max(logits, axis=0, keepdims=True)
        mybuf[d * NY + m, 1:2, :] = top + jnp.log(
            jnp.sum(jnp.exp(logits - top), axis=0, keepdims=True))
        picked0 = jnp.sum(jnp.where(expert_iota == ei[0:1, :], logits, 0.0), axis=0, keepdims=True)
        picked1 = jnp.sum(jnp.where(expert_iota == ei[1:2, :], logits, 0.0), axis=0, keepdims=True)
        higher = jnp.maximum(picked0, picked1)
        power0 = jnp.exp(picked0 - higher)
        power1 = jnp.exp(picked1 - higher)
        weight0 = power0 / (power0 + power1)
        weight1 = power1 / (power0 + power1)
        chunk_iota = lax.broadcasted_iota(jnp.int32, (LANE, TOK), 0)
        for j in range(NZ * CAP // LANE):
            rows = chunk_iota + j * LANE
            mixed = jnp.where(rows == flat0, weight0, 0.0) + jnp.where(rows == flat1, weight1, 0.0)
            mixed = mixed.T
            high = mixed.astype(BF16)
            chi[:, j * LANE:(j + 1) * LANE] = high
            clo[:, j * LANE:(j + 1) * LANE] = (mixed - high.astype(F32)).astype(BF16)

    def clear():
        acc_h[...] = jnp.zeros_like(acc_h)
        squares[...] = jnp.zeros_like(squares)
        acc_g[...] = jnp.zeros_like(acc_g)
        acc_u[...] = jnp.zeros_like(acc_u)

    def gain():
        @pl.loop(0, 512 // 16)
        def _(i):
            part = pl.ds(pl.multiple_of(i * 16, 16), 16)
            hw[part, :] = (hw[part, :].astype(F32) * fg[...]).astype(BF16)

    def gate_up_near():
        @pl.loop(0, 2)
        def _(k):
            gate_up((m + 1 + 2 * k) % NY, 0)

    a_leads = [(("g", j), k) for j in range(4) for k in (1, 2)]
    a_rest = [((("g", j), t), 1) for j in range(4) for t in range(3)]
    plan.work("router start", 0.05, [("slots", 1)], router_start)
    plan.arrives("router z", ["router start"], 6.5, lambda: wait(
        "router z", zbuf.at[pl.ds(0, NZ - 1)]))
    plan.work("swap", 0.1, ["router start"], swap_weights)
    plan.arrives("weights", ["swap"], 12.0, lambda: wait("weights", w3.at[:, pl.ds(HID, HID)]))
    plan.work("router middle", 0.1, ["router z"], router_middle)
    plan.arrives("router y", ["router middle"], 6.0, lambda: wait(
        "router y", ybuf.at[pl.ds(0, NY - 1)]))
    plan.work("router end", 0.4, ["router y"], router_end)
    plan.arrives("inverse", ["router end"], 6.0, lambda: wait(
        "inverse", ibuf.at[pl.ds(0, NX - 1)]))
    plan.work("gates", 0.4, ["router end"], gates)
    plan.work("clear", 0.1, [], clear)
    plan.work("gain", 0.85, ["swap"], gain)
    plan.work("gate up own", 0.72, ["clear", "weights"] + a_leads, lambda: gate_up(m, 0))
    plan.work("gate up near", 1.44, ["gate up own"] + a_rest, gate_up_near)
    plan.run()

    phase("gateup")

    blocks = [(at("y", 2), j) for j in range(4)]
    blocks += [(yy, j) for yy in range(NY) for j in range(4, NZ)]
    held = jnp.concatenate([xs[yy, :, j].reshape(ROWS, LANE) for yy, j in blocks], axis=1)
    for acc, weight in ((acc_g, gw), (acc_u, uw)):
        against = jnp.concatenate([columns(weight, e + j, yy) for yy, j in blocks], axis=1)
        acc[...] += lax.dot_general(held, against, LAST, preferred_element_type=F32)

    for xx in range(NX):
        rows = pl.ds(xx * CAP, CAP)
        scale = jnp.broadcast_to(ibuf[xx, 0:1, :], (LANE, LANE)).T[0:CAP, 0:1]
        gate_value = acc_g[rows, :] * scale
        up_value = acc_u[rows, :] * scale
        hid[rows, :] = (gate_value / (1.0 + jnp.exp(-gate_value)) * up_value).astype(BF16)

    phase("down")
    def down(yy, first):
        against = jnp.concatenate([columns(dw, e + first + j, yy) for j in range(4)], axis=1)
        product = jnp.dot(hid[...], against, preferred_element_type=F32).astype(BF16)
        for j in range(4):
            for xx in range(NX):
                ps[yy, xx, first + j] = product[
                    xx * CAP:(xx + 1) * CAP, j * LANE:(j + 1) * LANE
                ]

    def partial(yy, xx, j, part):
        if part is None:
            return ps.at[yy, xx, j]
        return ps.at[yy, xx, j, pl.ds(half * part, half)]

    def add_into(target, source):
        target[...] = (target[...].astype(F32) + source[...].astype(F32)).astype(BF16)

    plan = Plan()

    def reduce(tag, axis, units, starts, middles, ends):
        names = (tag, 1), (tag, 2)

        def add():
            for view, near, _, _ in units:
                for number, toward in enumerate((1, -1)):
                    add_into(view(at(axis, toward), number), near.at[number])

        def end():
            for view, _, far, into in units:
                into[...] = (view(coord[axis])[...].astype(F32) + far[0].astype(F32)
                             + far[1].astype(F32)).astype(BF16)

        for number, toward in enumerate((1, -1)):
            link = axis + "+-"[number]
            for view, near, far, _ in units:
                plan.send(names[0], link, piece / 2, starts,
                          lambda v=view, n=near, k=number, w=toward: send(
                    names[0], v(at(axis, 2), k), n.at[k], device(axis, w)))
                plan.send(names[1], link, piece, [(tag, "add")],
                          lambda v=view, f=far, k=number, w=toward: send(
                    names[1], v(at(axis, w)), f.at[k], device(axis, w)))
        count = len(units)
        plan.wait(names[0], lambda: wait(names[0], ps.at[0, 0, pl.ds(0, count)]))
        plan.wait(names[1], lambda: wait(names[1], ps.at[0, 0, pl.ds(0, 2 * count)]))
        plan.work((tag, "add"), 0.05 * count, [names[0]] + middles, add)
        plan.work((tag, "end"), 0.05 * count, [names[1]] + ends, end)

    def reduce_straight(tag, axis, view, far, into, firsts, seconds, ends):
        def end():
            total = view(coord[axis])[...].astype(F32)
            for number in range(3):
                total = total + far[number].astype(F32)
            into[...] = total.astype(BF16)

        plan.send_both((tag, 2), axis, piece, firsts, lambda: send(
            (tag, 2), view(at(axis, 2)), far.at[2], device(axis, 2)), 2)
        for number, toward in enumerate((1, -1)):
            plan.send((tag, 2), axis + "+-"[number], piece, seconds,
                      lambda k=number, w=toward: send(
                (tag, 2), view(at(axis, w)), far.at[k], device(axis, w)))
        plan.wait((tag, 2), lambda: wait((tag, 2), ps.at[0, 0, pl.ds(0, 3)]))
        plan.work((tag, "end"), 0.05, [(tag, 2)] + ends, end)

    for j in (0, 1, 2, 3, 4, 5, 6, 7):
        lead, rest = ("y", "x") if j < 4 else ("x", "y")

        def unit_of(t, j=j, lead=lead, rest=rest):
            if lead == "y":
                view = lambda s, p=None: partial(s, at("x", t), j, p)
            else:
                view = lambda s, p=None: partial(at("y", t), s, j, p)
            return view, near1.at[j, t % 4], far1.at[j, t % 4], sums.at[j, at(rest, t)]

        def sum_view(s, p=None, j=j):
            return sums.at[j, s] if p is None else sums.at[j, s, pl.ds(half * p, half)]

        for t, steps in ((2, (2,)), (1, (1, -1)), (0, (0,))):
            if lead == "y":
                starts, middles, ends = [("down", 0, 2)], [("down", 0, 1), ("down", 0, 3)], [
                    ("down", 0, 0)]
            else:
                starts = [("down", 4, step % 4) for step in steps]
                middles, ends = [], []
            reduce(("r", j, t), lead, [unit_of(step) for step in steps], starts, middles, ends)
        last = [[(("r", j, t), "end")] for t in (2, 1, 0)]
        if j in (0, 1, 6, 7):
            reduce_straight(("s", j), rest, sum_view, far2.at[j], fin.at[j], *last)
        else:
            reduce(("s", j), rest, [(sum_view, near2.at[j], far2.at[j], fin.at[j])], *last)
        if j > 0:
            hops = min(j, NZ - j)
            back = lambda j=j: send("back", fin.at[j], rx.at[e], device("z", j))
            if j == 4:
                plan.send_both("back", "z", piece, [(("s", j), "end")], back, hops)
            else:
                plan.send("back", "z+" if j < 4 else "z-", piece, [(("s", j), "end")], back, hops)
    plan.wait("back", lambda: wait("back", rx.at[pl.ds(0, NZ - 1)]))
    for first, step in ((0, 2), (4, 2), (4, 1), (4, 3), (0, 1), (0, 3), (4, 0), (0, 0)):
        plan.work(("down", first, step), 0.45, [],
                  lambda f=first, t=step: down(at("y", t), f))
    plan.run()
    phase("back")
    rx[e] = fin[0]
    phase("combine")
    outputs = rx[...].reshape(NZ * CAP, LANE)
    combined = jnp.dot(chi[...], outputs, preferred_element_type=F32)
    combined += jnp.dot(clo[...], outputs, preferred_element_type=F32)
    layer_out = (tk[...].astype(F32) + combined).astype(BF16)
    out_ref[...] = layer_out
    hs[m, e] = layer_out

    phase("head_gather")
    def rows_a(yy, zz, part=None):
        if part is None:
            return hs.at[yy, zz, pl.ds(0, CUT_A)]
        return hs.at[yy, zz, pl.ds(0, SUB_A)] if part == 0 else hs.at[
            yy, zz, pl.ds(SUB_A, CUT_A - SUB_A)]

    def rows_b(yy, zz, part=None):
        if part is None:
            return hs.at[yy, zz, pl.ds(CUT_A, CUT_B - CUT_A)]
        return hs.at[yy, zz, pl.ds(CUT_A, SUB_B - CUT_A)] if part == 0 else hs.at[
            yy, zz, pl.ds(SUB_B, CUT_B - SUB_B)]

    def ring8(rounds, start, tag, view, times):
        def begin():
            for k in (2, 1):
                for toward in (1, -1):
                    send((tag, k), view(e), view(e), device("z", toward * k))

        def step():
            wait((tag, 2), times(2))
            for toward, part in ((1, 0), (-1, 1)):
                source = at("z", -toward * 2)
                unit = view(source, part)
                send((tag, 3), unit, unit, device("z", toward * 2))
                send((tag, 3), view(source), view(source), device("z", toward))
            wait((tag, 1), times(2))

        def finish():
            wait((tag, 3), times(3))

        for number, event in enumerate((begin, step, finish)):
            rounds.setdefault(start + number, []).append(event)

    def logits_chunk(yy):
        held = jnp.concatenate([hs[yy, zz] for zz in range(NZ)], axis=1)
        against = jnp.concatenate([columns(hw, zz, yy) for zz in range(NZ)], axis=1)
        acc_h[...] += lax.dot_general(against, held, LAST, preferred_element_type=F32)
        total = squares[...]
        for zz in range(NZ):
            block = hs[yy, zz].astype(F32)
            total = total + block * block
        squares[...] = total

    def play(rounds, number):
        for event in rounds.get(number, []):
            event()

    def ring4(rounds, start, tag, axis, view, two):
        def begin():
            for toward in (1, -1):
                send((tag, 1), view(coord[axis]), view(coord[axis]), device(axis, toward))

        def step():
            wait((tag, 1), two)
            for toward, part in ((1, 0), (-1, 1)):
                unit = view(at(axis, -toward), part)
                send((tag, 2), unit, unit, device(axis, toward))

        def finish():
            wait((tag, 2), view(at(axis, 2)))

        for number, event in enumerate((begin, step, finish)):
            rounds.setdefault(start + number, []).append(event)

    head = {}
    ring4(head, 0, "hb y", "y", lambda s, p=None: rows_b(s, e, p),
         hs.at[m, pl.ds(0, 2), pl.ds(CUT_A, CUT_B - CUT_A)])
    ring8(head, 0, "ha z", lambda s, p=None: rows_a(m, s, p),
          lambda n: hs.at[m, pl.ds(0, n), pl.ds(0, CUT_A)])
    for start, near, far in ((2, (3, -3, 4), (2,)), (1, (1, -1, 2, -2), (1, -1)), (0, (0,), (0,))):
        for t in far:
            ring8(head, start, ("hb z", t), lambda s, p=None, t=t: rows_b(at("y", t), s, p),
                  lambda n, t=t: hs.at[at("y", t), pl.ds(0, n), pl.ds(CUT_A, CUT_B - CUT_A)])
        for t in near:
            ring4(head, start, ("ha y", t), "y", lambda s, p=None, t=t: rows_a(s, at("z", t), p),
                 hs.at[m, pl.ds(0, 2), pl.ds(0, CUT_A)])
    play(head, 0)
    play(head, 1)
    play(head, 2)

    logits_chunk(m)
    play(head, 3)

    @pl.loop(0, 2)
    def _(k):
        logits_chunk((m + 1 + 2 * k) % NY)

    play(head, 4)
    phase("logits")
    logits_chunk(at("y", 2))
    high = squares[...].astype(BF16)
    low = (squares[...] - high.astype(F32)).astype(BF16)
    ones16 = jnp.ones((16, LANE), BF16)
    total = lax.dot_general(ones16, high, LAST, preferred_element_type=F32)
    total += lax.dot_general(ones16, low, LAST, preferred_element_type=F32)
    head_scale = lax.rsqrt(total[0:1, :] / WIDTH + EPSILON)
    vocab = acc_h[...] * head_scale

    def logsum(rows):
        top = jnp.max(rows, axis=0, keepdims=True)
        return top + jnp.log(jnp.sum(jnp.exp(rows - top), axis=0, keepdims=True))

    def merged(rows):
        top = rows[0]
        for row in rows[1:]:
            top = jnp.maximum(top, row)
        whole = jnp.exp(rows[0] - top)
        for row in rows[1:]:
            whole = whole + jnp.exp(row - top)
        return top + jnp.log(whole)

    mzbuf[e] = logsum(vocab)
    phase("merge_z")
    for k in (4, 3, 5, 2, 6, 1, 7):
        send("merge z", mzbuf.at[e], mzbuf.at[e], device("z", k))
    wait("merge z", mzbuf.at[pl.ds(0, NZ - 1)])
    mybuf[d * NY + m, 0:1, :] = merged([mzbuf[k] for k in range(NZ)])
    phase("merge_xy")
    for step in others:
        send("merge xy", mybuf.at[d * NY + m], mybuf.at[d * NY + m], plane(*step))
    wait("merge xy", mybuf.at[pl.ds(0, len(others))])
    phase("penalty")
    router_sum = jnp.zeros((1, TOK), F32)
    head_sum = jnp.zeros((1, TOK), F32)
    for dp in range(2 * NX):
        routed = mybuf[dp * NY, 1:2, :]
        router_sum = router_sum + routed * routed
        ended = merged([mybuf[dp * NY + yy, 0:1, :] for yy in range(NY)])
        head_sum = head_sum + ended * ended
    lse_ref[...] = merged([mybuf[d * NY + yy, 0:1, :] for yy in range(NY)])

    def spread(row):
        return jnp.broadcast_to(jnp.sum(row, axis=1, keepdims=True), (1, LANE))

    rp_ref[...] = spread(router_sum) / (2 * NX * TOK)
    hp_ref[...] = spread(head_sum) / (2 * NX * TOK)

    phase("drain")
    for copy in sent[-SENDS:]:
        copy.wait_send()
    phase("")
    assert len(ids) == ARRIVALS


def body(tokens, expert_index, slot_index, norm_gain, router_weight, gate_weight, up_weight,
         down_weight, final_gain, head_weight):
    vmem = pl.BlockSpec(memory_space=pltpu.VMEM)
    hbm = pl.BlockSpec(memory_space=pl.ANY)
    scratch = [
        pltpu.VMEM((TOK, LANE), BF16),
        pltpu.VMEM((2, TOK), jnp.int32),
        pltpu.VMEM((2, TOK), jnp.int32),
        pltpu.VMEM((1, LANE), F32),
        pltpu.VMEM((8, LANE), BF16),
        pltpu.VMEM((1, WIDTH), F32),
        pltpu.VMEM((3, HID2, WIDTH), BF16),
        pltpu.VMEM((512, WIDTH), BF16),
        pltpu.VMEM((NZ, CAP, LANE), BF16),
        pltpu.VMEM((NY, NX, NZ, CAP, LANE), BF16),
        pltpu.VMEM((ROWS, HID2), F32),
        pltpu.VMEM((ROWS, HID2), F32),
        pltpu.VMEM((ROWS, HID2), BF16),
        pltpu.VMEM((NY, NX, NZ, CAP, LANE), BF16),
        pltpu.VMEM((NZ, 4, 2, CAP // 2, LANE), BF16),
        pltpu.VMEM((NZ, 4, 2, CAP, LANE), BF16),
        pltpu.VMEM((NZ, 4, CAP, LANE), BF16),
        pltpu.VMEM((NZ, 2, CAP // 2, LANE), BF16),
        pltpu.VMEM((NZ, 3, CAP, LANE), BF16),
        pltpu.VMEM((NZ, CAP, LANE), BF16),
        pltpu.VMEM((NZ, CAP, LANE), BF16),
        pltpu.VMEM((TOK, NZ * CAP), BF16),
        pltpu.VMEM((TOK, NZ * CAP), BF16),
        pltpu.VMEM((NY, NZ, TOK, LANE), BF16),
        pltpu.VMEM((512, TOK), F32),
        pltpu.VMEM((TOK, LANE), F32),
        pltpu.VMEM((NZ, 16, TOK), F32),
        pltpu.VMEM((NY, 16, TOK), F32),
        pltpu.VMEM((8, TOK), F32),
        pltpu.VMEM((NX, 8, LANE), F32),
        pltpu.VMEM((NZ, 1, TOK), F32),
        pltpu.VMEM((2 * NX * NY, 2, TOK), F32),
        pltpu.SemaphoreType.DMA((SENDS,)),
        pltpu.SemaphoreType.DMA((ARRIVALS,)),
        pltpu.SemaphoreType.DMA((10,)),
    ]
    layer_out, head_logsum, router_penalty, head_penalty = pl.pallas_call(
        kernel,
        name="layer",
        out_shape=(
            jax.ShapeDtypeStruct((TOK, LANE), BF16),
            jax.ShapeDtypeStruct((1, TOK), F32),
            jax.ShapeDtypeStruct((1, LANE), F32),
            jax.ShapeDtypeStruct((1, LANE), F32),
        ),
        in_specs=[hbm] * 10,
        out_specs=(vmem,) * 4,
        scratch_shapes=scratch,
        compiler_params=pltpu.CompilerParams(
            collective_id=0, has_side_effects=True, vmem_limit_bytes=56 * 1024 * 1024
        ),
    )(
        tokens, expert_index.T, slot_index.T, norm_gain[None, :], router_weight,
        final_gain[None, :], gate_weight[0], up_weight[0], down_weight[0], head_weight,
    )
    return layer_out, head_logsum[0], router_penalty[0, 0], head_penalty[0, 0]


def solution(mesh):
    in_specs = (
        P("dp", ("expert", "mp")),
        P("dp", None),
        P("dp", None),
        P(("expert", "mp")),
        P(None, ("expert", "mp")),
        P("expert", ("dp", "mp"), None),
        P("expert", ("dp", "mp"), None),
        P("expert", ("dp", "mp"), None),
        P(),
        P(("expert", "mp"), None),
    )
    out_specs = (P("dp", ("expert", "mp")), P("dp"), P(), P())
    return jax.shard_map(body, mesh=mesh, in_specs=in_specs, out_specs=out_specs, check_vma=False)
```

```python
import jax
import jax.numpy as jnp
from jax import lax
from jax.experimental import pallas as pl
from jax.experimental.pallas import tpu as pltpu
from jax.sharding import PartitionSpec as P

F32 = jnp.float32
BF16 = jnp.bfloat16
EPSILON = 1e-05
LAST = (((1,), (1,)), ((), ()))
EXACT = lax.Precision.HIGHEST

NX, NY, NZ = 4, 4, 8
CAP = 96
TOK = 256
LANE = 128
HID = 224
HID2 = 2 * HID
WIDTH = LANE * NY * NZ
ROWS = NX * CAP
LOTS = 11
ARRIVALS = 138
CUT_A, CUT_B = 176, 256
SUB_A, SUB_B = 96, 224


class Plan:
    RATE, FIRST, HOP = 46.6e3, 2.6, 0.75

    def __init__(self):
        self.sends, self.works, self.waits, self.given = [], [], {}, {}

    def send(self, group, link, size, needs, emit, hops=1):
        self.sends.append([group, link, size / self.RATE, frozenset(needs), emit, hops])

    def send_both(self, group, axis, size, needs, emit, hops):
        self.send(group, axis + "+", size / 2, needs, emit, hops)
        self.send(group, axis + "-", size / 2, needs, lambda: None, hops)

    def wait(self, group, emit):
        self.waits[group] = emit

    def arrives(self, group, needs, delay, emit):
        self.given[group] = (frozenset(needs), delay)
        self.waits[group] = emit

    def work(self, name, time, needs, emit):
        self.works.append([name, time, frozenset(needs), emit])

    def chains(self):
        after = {}
        for group, _, time, needs, _, hops in self.sends:
            for need in needs:
                after.setdefault(need, []).append(
                    (time + self.FIRST + self.HOP * (hops - 1), group))
        for name, time, needs, _ in self.works:
            for need in needs:
                after.setdefault(need, []).append((time, name))
        for group, (needs, delay) in self.given.items():
            for need in needs:
                after.setdefault(need, []).append((delay, group))
        memo = {}

        def rest(event):
            if event not in memo:
                memo[event] = max((t + rest(n) for t, n in after.get(event, [])), default=0.0)
            return memo[event]

        return rest

    def run(self):
        horizons = (0.3, 0.5, 0.7, 1.0, 1.5)
        return self.play(min(horizons, key=lambda h: self.play(h, False)))

    def play(self, horizon, real=True):
        rest = self.chains()
        clock, free, had = 0.0, {}, set()
        sends, works = list(self.sends), list(self.works)
        left, when, due, done = {}, {}, {}, set()
        for item in sends:
            left[item[0]] = left.get(item[0], 0) + 1

        def issue(force):
            nonlocal sends
            ready = [item for item in sends if item[3] <= had]
            ready.sort(key=lambda item: -(item[2] + rest(item[0])))
            gone = []
            for item in ready:
                group, link, time, _, emit, hops = item
                if free.get(link, 0.0) > clock + horizon and not force:
                    continue
                if real:
                    emit()
                free[link] = max(clock, free.get(link, 0.0)) + time * hops
                arrival = free[link] + self.FIRST + self.HOP * (hops - 1)
                when[group] = max(when.get(group, 0.0), arrival)
                left[group] -= 1
                if left[group] == 0:
                    due[group] = when[group]
                gone.append(id(item))
            sends = [item for item in sends if id(item) not in gone]

        while True:
            for group, (needs, delay) in self.given.items():
                if group not in due and needs <= had:
                    due[group] = clock + delay
            issue(False)
            coming = sorted((time, str(group), group) for group, time in due.items()
                            if group not in done)
            ready = [item for item in works if item[2] <= had]
            ready.sort(key=lambda item: -(item[1] + rest(item[0])))
            chosen = None
            for item in ready:
                if not coming or coming[0][0] - clock >= 0.6 * item[1] or (
                        rest(item[0]) + item[1] > rest(coming[0][2]) + 1.0):
                    chosen = item
                    break
            if chosen is not None:
                works = [item for item in works if item is not chosen]
                if real:
                    chosen[3]()
                clock += chosen[1]
                had.add(chosen[0])
            elif coming:
                time, _, group = coming[0]
                if real:
                    self.waits[group]()
                clock = max(clock, time) + 0.01
                done.add(group)
                had.add(group)
            elif sends:
                issue(True)
            else:
                break
        return clock


def kernel(
    tk_h, ei_h, si_h, ng_h, rw_h, fg_h, gw_h, uw_h, dw_h, hw_h,
    out_ref, lse_ref, rp_ref, hp_ref,
    tk, ei, si, ng, rw, fg,
    w3, hw, ls, xs, acc_g, acc_u, hid, ps, near1, far1,
    sums, near2, far2, fin, rx, chi, clo, hs, acc_h, squares,
    zbuf, ybuf, rbuf, ibuf, mzbuf, mybuf, ssem, rsem, lsem,
):
    d = lax.axis_index("dp")
    e = lax.axis_index("expert")
    m = lax.axis_index("mp")
    x = d // 2
    c = d % 2
    gw, uw, dw = w3.at[0], w3.at[1], w3.at[2]
    coord = {"x": x, "y": m, "z": e}
    extent = {"x": NX, "y": NY, "z": NZ}

    def at(axis, step):
        return (coord[axis] + step + extent[axis]) % extent[axis]

    def device(axis, step):
        if axis == "x":
            return {"dp": at("x", step) * 2 + c, "expert": e, "mp": m}
        if axis == "y":
            return {"dp": d, "expert": e, "mp": at("y", step)}
        return {"dp": d, "expert": at("z", step), "mp": m}

    def plane(step_x, step_y, other):
        dp = at("x", step_x) * 2 + (1 - c if other else c)
        return {"dp": dp, "expert": e, "mp": at("y", step_y)}

    ids = {}
    sent = {}
    lots = {"now": None}
    scopes = []

    def phase(name):
        while scopes:
            scopes.pop().__exit__(None, None, None)
        if name:
            scopes.append(jax.named_scope(name))
            scopes[-1].__enter__()


    def remote(tag, slot, src, dst, dev):
        number = ids.setdefault(tag, len(ids))
        return pltpu.make_async_remote_copy(
            src_ref=src, dst_ref=dst, send_sem=ssem.at[slot], recv_sem=rsem.at[number],
            device_id=dev, device_id_type=pl.DeviceIdType.MESH,
        )

    def send(tag, src, dst, dev):
        lot = lots["now"] or (tag[0] if isinstance(tag, tuple) else tag)
        sent.setdefault(lot, len(sent))
        remote(tag, sent[lot], src, dst, dev).start()

    def send_in(lot, *copy):
        lots["now"] = lot
        send(*copy)
        lots["now"] = None

    def wait(tag, ref):
        remote(tag, 0, ref, ref, device("y", 1)).wait_recv()

    phase("entry")
    smalls = [
        pltpu.make_async_copy(source, held, lsem.at[4 + number])
        for number, (source, held) in enumerate(
            ((tk_h, tk), (ei_h, ei), (si_h, si), (ng_h, ng), (rw_h, rw), (fg_h, fg))
        )
    ]
    loads = [
        pltpu.make_async_copy(gw_h, gw.at[pl.ds(0, HID)], lsem.at[0]),
        pltpu.make_async_copy(uw_h, uw.at[pl.ds(0, HID)], lsem.at[1]),
        pltpu.make_async_copy(dw_h, dw.at[pl.ds(0, HID)], lsem.at[2]),
        pltpu.make_async_copy(hw_h, hw, lsem.at[3]),
    ]
    barrier = pltpu.get_barrier_semaphore()
    partners = [device("z", k) for k in range(1, NZ)]
    others = [
        (step_x, step_y, other)
        for step_x in (2, 1, 3, 0) for step_y in (2, 1, 3, 0) for other in (True, False)
        if (step_x, step_y, other) != (0, 0, False)
    ]
    partners += [plane(*step) for step in others]
    for partner in partners:
        pl.semaphore_signal(
            barrier, inc=1, device_id=partner, device_id_type=pl.DeviceIdType.MESH
        )

    phase("choose")
    for load in smalls + loads:
        load.start()
    for load in smalls:
        load.wait()

    t32 = tk[...].astype(F32)
    gained = (t32 * ng[...]).astype(BF16)
    flat0 = ei[0:1, :] * CAP + si[0:1, :]
    flat1 = ei[1:2, :] * CAP + si[1:2, :]
    slot_iota = lax.broadcasted_iota(jnp.int32, (CAP, TOK), 0)
    for ex in range(NZ):
        rows = slot_iota + ex * CAP
        choose = jnp.where((rows == flat0) | (rows == flat1), 1.0, 0.0).astype(BF16)
        ls[ex] = jnp.dot(choose, gained, preferred_element_type=F32).astype(BF16)
    router_gained = rw[...].astype(F32) * ng[...]
    zbuf[e, 0:8, :] = lax.dot_general(
        router_gained, t32, LAST, precision=EXACT, preferred_element_type=F32
    )
    ones8 = jnp.ones((8, LANE), F32)
    zbuf[e, 8:16, :] = lax.dot_general(
        ones8, t32 * t32, LAST, precision=EXACT, preferred_element_type=F32
    )
    xs[m, x, 0] = ls[e]

    phase("barrier")
    pl.semaphore_wait(barrier, len(partners))
    for k in (1, 7, 2, 6, 3, 5, 4):
        send(("slots", min(k, NZ - k)), ls.at[at("z", k)], xs.at[m, x, NZ - k], device("z", k))
    piece = CAP * LANE * 2
    half = CAP // 2

    def slab(yy, xx, j, part=None):
        if part is None:
            return xs.at[yy, xx, j]
        return xs.at[yy, xx, j, pl.ds(half * part, half)]

    plan = Plan()
    phase("gather")

    def ring(plan, tag, axis, size, views, needs, two, one, last=None):
        end = last or (tag, 2)
        for number, toward in enumerate((1, -1)):
            link = axis + "+-"[number]
            for view in views:
                plan.send((tag, 1), link, size, needs, lambda v=view, w=toward: send_in(
                    "gather", (tag, 1), v(coord[axis]), v(coord[axis]), device(axis, w)))
                plan.send(end, link, size / 2, [(tag, 1)],
                          lambda v=view, w=toward, p=number: send_in(
                    "gather", end, v(at(axis, -w), p), v(at(axis, -w), p), device(axis, w)))
        plan.wait((tag, 1), lambda: wait((tag, 1), two))
        if last is None:
            plan.wait(end, lambda: wait(end, one))

    for k, time in ((1, 3.3), (2, 4.5), (3, 6.0), (4, 7.2)):
        plan.arrives(("slots", k), [], time, lambda k=k: wait(
            ("slots", k), xs.at[m, x, pl.ds(0, 1 if k == 4 else 2)]))
    for j in (0, 7, 1, 6, 2, 5, 3, 4):
        lead, rest = ("x", "y") if j < 4 else ("y", "x")

        def view_of(t, j=j, lead=lead):
            if lead == "x":
                return lambda s, p=None: slab(s, at("x", t), j, p)
            return lambda s, p=None: slab(at("y", t), s, j, p)

        def lead_view(s, p=None, j=j, lead=lead):
            return slab(m, s, j, p) if lead == "x" else slab(s, x, j, p)

        near = [("slots", min(j, NZ - j))] if j > 0 else []
        tag = ("g", j)
        ring(plan, tag, lead, piece, [lead_view], near, xs.at[0, 0, pl.ds(0, 2)], xs.at[0, 0, 0])
        ring(plan, (tag, 0), rest, piece, [view_of(0)], near,
             xs.at[0, 0, pl.ds(0, 2)], None, "gather end")
        ring(plan, (tag, 1), rest, piece, [view_of(1), view_of(-1)], [(tag, 1)],
             xs.at[0, 0, pl.ds(0, 4)], None, "gather end")
        ring(plan, (tag, 2), rest, piece, [view_of(2)], [(tag, 2)],
             xs.at[0, 0, pl.ds(0, 2)], None, "gather end")

    plan.wait("gather end", lambda: wait("gather end", ps.at[pl.ds(0, 4)]))

    def columns(weight, ex, yy):
        block = (ex % NZ) * NY + yy
        return weight[:, pl.ds(pl.multiple_of(block * LANE, LANE), LANE)]

    def gate_up(yy, first):
        held = jnp.concatenate([xs[yy, :, first + j].reshape(ROWS, LANE) for j in range(4)], axis=1)
        for acc, weight in ((acc_g, gw), (acc_u, uw)):
            against = jnp.concatenate([columns(weight, e + first + j, yy) for j in range(4)], axis=1)
            acc[...] += lax.dot_general(held, against, LAST, preferred_element_type=F32)

    def gate_up_rows(steps):
        blocks = [(yy, j) for yy in range(NY) for j in range(4, NZ)]
        held = jnp.concatenate([jnp.concatenate(
            [xs[yy, at("x", t), j] for yy, j in blocks], axis=1) for t in steps], axis=0)
        for acc, weight in ((acc_g, gw), (acc_u, uw)):
            against = jnp.concatenate([columns(weight, e + j, yy) for yy, j in blocks], axis=1)
            product = lax.dot_general(held, against, LAST, preferred_element_type=F32)
            for number, t in enumerate(steps):
                rows = pl.ds(pl.multiple_of(at("x", t) * CAP, CAP), CAP)
                acc[rows, :] += product[number * CAP:(number + 1) * CAP]

    def swap_weights():
        for load in loads:
            load.wait()
        send("weights", w3.at[:, pl.ds(0, HID)], w3.at[:, pl.ds(HID, HID)], plane(0, 0, True))

    def router_start():
        for k in range(1, NZ):
            send("router z", zbuf.at[e], zbuf.at[e], device("z", k))

    def router_middle():
        total = zbuf[0]
        for k in range(1, NZ):
            total = total + zbuf[k]
        ybuf[m] = total
        for k in range(1, NY):
            send("router y", ybuf.at[m], ybuf.at[m], device("y", k))

    def router_end():
        total = ((ybuf[0] + ybuf[1]) + ybuf[2]) + ybuf[3]
        inverse8 = lax.rsqrt(total[8:16] / WIDTH + EPSILON)
        rbuf[...] = total[0:8] * inverse8
        place = slot_iota + e * CAP
        mine = jnp.where((place == flat0) | (place == flat1), 1.0, 0.0)
        mine = jnp.concatenate([mine, jnp.zeros((LANE - CAP, TOK), F32)], axis=0)
        ibuf[x] = lax.dot_general(
            inverse8, mine, LAST, precision=EXACT, preferred_element_type=F32
        )
        for k in range(1, NX):
            send("inverse", ibuf.at[x], ibuf.at[x], device("x", k))

    def gates():
        logits = rbuf[...]
        expert_iota = lax.broadcasted_iota(jnp.int32, (8, TOK), 0)
        top = jnp.max(logits, axis=0, keepdims=True)
        mybuf[d * NY + m, 1:2, :] = top + jnp.log(
            jnp.sum(jnp.exp(logits - top), axis=0, keepdims=True))
        picked0 = jnp.sum(jnp.where(expert_iota == ei[0:1, :], logits, 0.0), axis=0, keepdims=True)
        picked1 = jnp.sum(jnp.where(expert_iota == ei[1:2, :], logits, 0.0), axis=0, keepdims=True)
        higher = jnp.maximum(picked0, picked1)
        power0 = jnp.exp(picked0 - higher)
        power1 = jnp.exp(picked1 - higher)
        weight0 = power0 / (power0 + power1)
        weight1 = power1 / (power0 + power1)
        chunk_iota = lax.broadcasted_iota(jnp.int32, (LANE, TOK), 0)
        for j in range(NZ * CAP // LANE):
            rows = chunk_iota + j * LANE
            mixed = jnp.where(rows == flat0, weight0, 0.0) + jnp.where(rows == flat1, weight1, 0.0)
            mixed = mixed.T
            high = mixed.astype(BF16)
            chi[:, j * LANE:(j + 1) * LANE] = high
            clo[:, j * LANE:(j + 1) * LANE] = (mixed - high.astype(F32)).astype(BF16)

    def clear():
        acc_h[...] = jnp.zeros_like(acc_h)
        squares[...] = jnp.zeros_like(squares)
        acc_g[...] = jnp.zeros_like(acc_g)
        acc_u[...] = jnp.zeros_like(acc_u)

    def gain():
        @pl.loop(0, 512 // 16)
        def _(i):
            part = pl.ds(pl.multiple_of(i * 16, 16), 16)
            hw[part, :] = (hw[part, :].astype(F32) * fg[...]).astype(BF16)

    def gate_up_near():
        @pl.loop(0, 2)
        def _(k):
            gate_up((m + 1 + 2 * k) % NY, 0)

    a_leads = [(("g", j), k) for j in range(4) for k in (1, 2)]
    a_rest = [((("g", j), t), 1) for j in range(4) for t in range(3)]
    plan.work("router start", 0.05, [("slots", 1)], router_start)
    plan.arrives("router z", ["router start"], 6.5, lambda: wait(
        "router z", zbuf.at[pl.ds(0, NZ - 1)]))
    plan.work("swap", 0.1, ["router start"], swap_weights)
    plan.arrives("weights", ["swap"], 12.0, lambda: wait("weights", w3.at[:, pl.ds(HID, HID)]))
    plan.work("router middle", 0.1, ["router z"], router_middle)
    plan.arrives("router y", ["router middle"], 6.0, lambda: wait(
        "router y", ybuf.at[pl.ds(0, NY - 1)]))
    plan.work("router end", 0.4, ["router y"], router_end)
    plan.arrives("inverse", ["router end"], 6.0, lambda: wait(
        "inverse", ibuf.at[pl.ds(0, NX - 1)]))
    plan.work("gates", 0.4, ["router end"], gates)
    plan.work("clear", 0.1, [], clear)
    plan.work("gain", 0.85, ["swap"], gain)
    plan.work("gate up own", 0.72, ["clear", "weights"] + a_leads, lambda: gate_up(m, 0))
    plan.work("gate up near", 1.44, ["gate up own"] + a_rest, gate_up_near)
    b_rest = [((("g", j), t), 1) for j in range(4, NZ) for t in range(3)]
    plan.work("gate up rows", 1.3, ["clear", "weights"] + b_rest, lambda: gate_up_rows((0, 1, -1)))
    plan.run()

    phase("gateup")

    gate_up_rows((2,))
    gate_up(at("y", 2), 0)

    for xx in range(NX):
        rows = pl.ds(xx * CAP, CAP)
        scale = jnp.broadcast_to(ibuf[xx, 0:1, :], (LANE, LANE)).T[0:CAP, 0:1]
        gate_value = acc_g[rows, :] * scale
        up_value = acc_u[rows, :] * scale
        hid[rows, :] = (gate_value / (1.0 + jnp.exp(-gate_value)) * up_value).astype(BF16)

    phase("down")
    def down(yy, first):
        against = jnp.concatenate([columns(dw, e + first + j, yy) for j in range(4)], axis=1)
        product = jnp.dot(hid[...], against, preferred_element_type=F32).astype(BF16)
        for j in range(4):
            for xx in range(NX):
                ps[yy * NX + xx, first + j] = product[
                    xx * CAP:(xx + 1) * CAP, j * LANE:(j + 1) * LANE
                ]

    def partial(yy, xx, j, part):
        if part is None:
            return ps.at[yy * NX + xx, j]
        return ps.at[yy * NX + xx, j, pl.ds(half * part, half)]

    def add_into(target, source):
        target[...] = (target[...].astype(F32) + source[...].astype(F32)).astype(BF16)

    plan = Plan()

    def reduce(tag, axis, units, starts, middles, ends):
        names = (tag, 1), (tag, 2)

        def add():
            for view, near, _, _ in units:
                for number, toward in enumerate((1, -1)):
                    add_into(view(at(axis, toward), number), near.at[number])

        def end():
            for view, _, far, into in units:
                into[...] = (view(coord[axis])[...].astype(F32) + far[0].astype(F32)
                             + far[1].astype(F32)).astype(BF16)

        for number, toward in enumerate((1, -1)):
            link = axis + "+-"[number]
            for view, near, far, _ in units:
                plan.send(names[0], link, piece / 2, starts,
                          lambda v=view, n=near, k=number, w=toward: send_in(
                    "reduce", names[0], v(at(axis, 2), k), n.at[k], device(axis, w)))
                plan.send(names[1], link, piece, [(tag, "add")],
                          lambda v=view, f=far, k=number, w=toward: send_in(
                    "reduce", names[1], v(at(axis, w)), f.at[k], device(axis, w)))
        count = len(units)
        plan.wait(names[0], lambda: wait(names[0], ps.at[0, pl.ds(0, count)]))
        plan.wait(names[1], lambda: wait(names[1], ps.at[0, pl.ds(0, 2 * count)]))
        plan.work((tag, "add"), 0.05 * count, [names[0]] + middles, add)
        plan.work((tag, "end"), 0.05 * count, [names[1]] + ends, end)

    def reduce_straight(tag, axis, view, far, into, firsts, seconds, ends):
        def end():
            total = view(coord[axis])[...].astype(F32)
            for number in range(3):
                total = total + far[number].astype(F32)
            into[...] = total.astype(BF16)

        plan.send_both((tag, 2), axis, piece, firsts, lambda: send_in(
                    "reduce", (tag, 2), view(at(axis, 2)), far.at[2], device(axis, 2)), 2)
        for number, toward in enumerate((1, -1)):
            plan.send((tag, 2), axis + "+-"[number], piece, seconds,
                      lambda k=number, w=toward: send_in(
                    "reduce", (tag, 2), view(at(axis, w)), far.at[k], device(axis, w)))
        plan.wait((tag, 2), lambda: wait((tag, 2), ps.at[0, pl.ds(0, 3)]))
        plan.work((tag, "end"), 0.05, [(tag, 2)] + ends, end)

    for j in (0, 1, 2, 3, 4, 5, 6, 7):
        lead, rest = ("y", "x") if j < 4 else ("x", "y")

        def unit_of(t, j=j, lead=lead, rest=rest):
            if lead == "y":
                view = lambda s, p=None: partial(s, at("x", t), j, p)
            else:
                view = lambda s, p=None: partial(at("y", t), s, j, p)
            return view, near1.at[j, t % 4], far1.at[j, t % 4], sums.at[j, at(rest, t)]

        def sum_view(s, p=None, j=j):
            return sums.at[j, s] if p is None else sums.at[j, s, pl.ds(half * p, half)]

        for t, steps in ((2, (2,)), (1, (1, -1)), (0, (0,))):
            if lead == "y":
                starts, middles, ends = [("down", 0, 2)], [("down", 0, 1), ("down", 0, 3)], [
                    ("down", 0, 0)]
            else:
                starts = [("down", 4, step % 4) for step in steps]
                middles, ends = [], []
            reduce(("r", j, t), lead, [unit_of(step) for step in steps], starts, middles, ends)
        last = [[(("r", j, t), "end")] for t in (2, 1, 0)]
        if j in (0, 1, 6, 7):
            reduce_straight(("s", j), rest, sum_view, far2.at[j], fin.at[j], *last)
        else:
            reduce(("s", j), rest, [(sum_view, near2.at[j], far2.at[j], fin.at[j])], *last)
        if j > 0:
            hops = min(j, NZ - j)
            back = lambda j=j: send("back", fin.at[j], rx.at[e], device("z", j))
            if j == 4:
                plan.send_both("back", "z", piece, [(("s", j), "end")], back, hops)
            else:
                plan.send("back", "z+" if j < 4 else "z-", piece, [(("s", j), "end")], back, hops)
    plan.wait("back", lambda: wait("back", rx.at[pl.ds(0, NZ - 1)]))
    for first, step in ((0, 2), (4, 2), (4, 1), (4, 3), (0, 1), (0, 3), (4, 0), (0, 0)):
        plan.work(("down", first, step), 0.45, [],
                  lambda f=first, t=step: down(at("y", t), f))
    plan.run()
    phase("back")
    rx[e] = fin[0]
    phase("combine")
    outputs = rx[...].reshape(NZ * CAP, LANE)
    combined = jnp.dot(chi[...], outputs, preferred_element_type=F32)
    combined += jnp.dot(clo[...], outputs, preferred_element_type=F32)
    layer_out = (tk[...].astype(F32) + combined).astype(BF16)
    out_ref[...] = layer_out
    hs[m * NZ + e] = layer_out

    phase("head_gather")
    def rows_a(yy, zz, part=None):
        if part is None:
            return hs.at[yy * NZ + zz, pl.ds(0, CUT_A)]
        return hs.at[yy * NZ + zz, pl.ds(0, SUB_A)] if part == 0 else hs.at[
            yy * NZ + zz, pl.ds(SUB_A, CUT_A - SUB_A)]

    def rows_b(yy, zz, part=None):
        if part is None:
            return hs.at[yy * NZ + zz, pl.ds(CUT_A, CUT_B - CUT_A)]
        return hs.at[yy * NZ + zz, pl.ds(CUT_A, SUB_B - CUT_A)] if part == 0 else hs.at[
            yy * NZ + zz, pl.ds(SUB_B, CUT_B - SUB_B)]

    def ring8(rounds, start, tag, view, times):
        def begin():
            for k in (2, 1):
                for toward in (1, -1):
                    send_in("head", (tag, k), view(e), view(e), device("z", toward * k))

        def step():
            wait((tag, 2), times(2))
            for toward, part in ((1, 0), (-1, 1)):
                source = at("z", -toward * 2)
                unit = view(source, part)
                send_in("head", (tag, 3), unit, unit, device("z", toward * 2))
                send_in("head", (tag, 3), view(source), view(source), device("z", toward))
            wait((tag, 1), times(2))

        def finish():
            wait((tag, 3), times(3))

        for number, event in enumerate((begin, step, finish)):
            rounds.setdefault(start + number, []).append(event)

    def logits_chunk(yy):
        held = jnp.concatenate([hs[yy * NZ + zz] for zz in range(NZ)], axis=1)
        against = jnp.concatenate([columns(hw, zz, yy) for zz in range(NZ)], axis=1)
        acc_h[...] += lax.dot_general(against, held, LAST, preferred_element_type=F32)
        total = squares[...]
        for zz in range(NZ):
            block = hs[yy * NZ + zz].astype(F32)
            total = total + block * block
        squares[...] = total

    def play(rounds, number):
        for event in rounds.get(number, []):
            event()

    def ring4(rounds, start, tag, axis, view, two, last=None):
        def begin():
            for toward in (1, -1):
                send_in("head", (tag, 1), view(coord[axis]), view(coord[axis]), device(axis, toward))

        def step():
            wait((tag, 1), two)
            for toward, part in ((1, 0), (-1, 1)):
                unit = view(at(axis, -toward), part)
                send_in("head", last or (tag, 2), unit, unit, device(axis, toward))

        def finish():
            if last is None:
                wait((tag, 2), view(at(axis, 2)))

        for number, event in enumerate((begin, step, finish)):
            rounds.setdefault(start + number, []).append(event)

    head = {}
    ring4(head, 0, "hb y", "y", lambda s, p=None: rows_b(s, e, p),
         hs.at[pl.ds(0, 2), pl.ds(CUT_A, CUT_B - CUT_A)])
    ring8(head, 0, "ha z", lambda s, p=None: rows_a(m, s, p),
          lambda n: hs.at[pl.ds(0, n), pl.ds(0, CUT_A)])
    for start, near, far in ((2, (3, -3, 4), (2,)), (1, (1, -1, 2, -2), (1, -1)), (0, (0,), (0,))):
        for t in far:
            ring8(head, start, ("hb z", t), lambda s, p=None, t=t: rows_b(at("y", t), s, p),
                  lambda n, t=t: hs.at[pl.ds(0, n), pl.ds(CUT_A, CUT_B - CUT_A)])
        for t in near:
            ring4(head, start, ("ha y", t), "y", lambda s, p=None, t=t: rows_a(s, at("z", t), p),
                 hs.at[pl.ds(0, 2), pl.ds(0, CUT_A)], "ha end")
    play(head, 0)
    play(head, 1)
    play(head, 2)

    logits_chunk(m)
    play(head, 3)

    @pl.loop(0, 2)
    def _(k):
        logits_chunk((m + 1 + 2 * k) % NY)

    play(head, 4)
    wait("ha end", hs.at[pl.ds(0, NZ), pl.ds(0, CUT_A)])
    phase("logits")
    logits_chunk(at("y", 2))
    high = squares[...].astype(BF16)
    low = (squares[...] - high.astype(F32)).astype(BF16)
    ones16 = jnp.ones((16, LANE), BF16)
    total = lax.dot_general(ones16, high, LAST, preferred_element_type=F32)
    total += lax.dot_general(ones16, low, LAST, preferred_element_type=F32)
    head_scale = lax.rsqrt(total[0:1, :] / WIDTH + EPSILON)
    vocab = acc_h[...] * head_scale

    def logsum(rows):
        top = jnp.max(rows, axis=0, keepdims=True)
        return top + jnp.log(jnp.sum(jnp.exp(rows - top), axis=0, keepdims=True))

    def merged(rows):
        top = rows[0]
        for row in rows[1:]:
            top = jnp.maximum(top, row)
        whole = jnp.exp(rows[0] - top)
        for row in rows[1:]:
            whole = whole + jnp.exp(row - top)
        return top + jnp.log(whole)

    mzbuf[e] = logsum(vocab)
    phase("merge_z")
    for k in (4, 3, 5, 2, 6, 1, 7):
        send("merge z", mzbuf.at[e], mzbuf.at[e], device("z", k))
    wait("merge z", mzbuf.at[pl.ds(0, NZ - 1)])
    mybuf[d * NY + m, 0:1, :] = merged([mzbuf[k] for k in range(NZ)])
    phase("merge_xy")
    for step in others:
        send("merge xy", mybuf.at[d * NY + m], mybuf.at[d * NY + m], plane(*step))
    wait("merge xy", mybuf.at[pl.ds(0, len(others))])
    phase("penalty")
    router_sum = jnp.zeros((1, TOK), F32)
    head_sum = jnp.zeros((1, TOK), F32)
    for dp in range(2 * NX):
        routed = mybuf[dp * NY, 1:2, :]
        router_sum = router_sum + routed * routed
        ended = merged([mybuf[dp * NY + yy, 0:1, :] for yy in range(NY)])
        head_sum = head_sum + ended * ended
    lse_ref[...] = merged([mybuf[d * NY + yy, 0:1, :] for yy in range(NY)])

    def spread(row):
        return jnp.broadcast_to(jnp.sum(row, axis=1, keepdims=True), (1, LANE))

    rp_ref[...] = spread(router_sum) / (2 * NX * TOK)
    hp_ref[...] = spread(head_sum) / (2 * NX * TOK)

    phase("drain")
    for lot, ref in (
        ("slots", ls.at[pl.ds(0, NZ - 1)]), ("router z", zbuf.at[pl.ds(0, NZ - 1)]),
        ("weights", w3.at[:, pl.ds(0, HID)]), ("router y", ybuf.at[pl.ds(0, NY - 1)]),
        ("inverse", ibuf.at[pl.ds(0, NX - 1)]), ("gather", ps.at[pl.ds(0, NX * NY - 1)]),
        ("reduce", ps.at[pl.ds(0, NX * NY - 1)]), ("back", fin.at[pl.ds(0, NZ - 1)]),
        ("head", hs.at[pl.ds(0, NY * NZ - 1)]), ("merge z", mzbuf.at[pl.ds(0, NZ - 1)]),
        ("merge xy", mybuf.at[pl.ds(0, len(others))]),
    ):
        remote(("slots", 1), sent[lot], ref, ref, device("y", 1)).wait_send()
    phase("")
    assert len(ids) == ARRIVALS and len(sent) == LOTS, (len(ids), len(sent))


def finish(*refs):
    sources, results, sem = refs[:4], refs[4:8], refs[8]
    copies = [pltpu.make_async_copy(source, result, sem.at[number])
              for number, (source, result) in enumerate(zip(sources, results))]
    for copy in copies:
        copy.start()
    for copy in copies:
        copy.wait()


def body(tokens, expert_index, slot_index, norm_gain, router_weight, gate_weight, up_weight,
         down_weight, final_gain, head_weight):
    vmem = pl.BlockSpec(memory_space=pltpu.VMEM)
    hbm = pl.BlockSpec(memory_space=pl.ANY)
    scratch = [
        pltpu.VMEM((TOK, LANE), BF16),
        pltpu.VMEM((2, TOK), jnp.int32),
        pltpu.VMEM((2, TOK), jnp.int32),
        pltpu.VMEM((1, LANE), F32),
        pltpu.VMEM((8, LANE), BF16),
        pltpu.VMEM((1, WIDTH), F32),
        pltpu.VMEM((3, HID2, WIDTH), BF16),
        pltpu.VMEM((512, WIDTH), BF16),
        pltpu.VMEM((NZ, CAP, LANE), BF16),
        pltpu.VMEM((NY, NX, NZ, CAP, LANE), BF16),
        pltpu.VMEM((ROWS, HID2), F32),
        pltpu.VMEM((ROWS, HID2), F32),
        pltpu.VMEM((ROWS, HID2), BF16),
        pltpu.VMEM((NY * NX, NZ, CAP, LANE), BF16),
        pltpu.VMEM((NZ, 4, 2, CAP // 2, LANE), BF16),
        pltpu.VMEM((NZ, 4, 2, CAP, LANE), BF16),
        pltpu.VMEM((NZ, 4, CAP, LANE), BF16),
        pltpu.VMEM((NZ, 2, CAP // 2, LANE), BF16),
        pltpu.VMEM((NZ, 3, CAP, LANE), BF16),
        pltpu.VMEM((NZ, CAP, LANE), BF16),
        pltpu.VMEM((NZ, CAP, LANE), BF16),
        pltpu.VMEM((TOK, NZ * CAP), BF16),
        pltpu.VMEM((TOK, NZ * CAP), BF16),
        pltpu.VMEM((NY * NZ, TOK, LANE), BF16),
        pltpu.VMEM((512, TOK), F32),
        pltpu.VMEM((TOK, LANE), F32),
        pltpu.VMEM((NZ, 16, TOK), F32),
        pltpu.VMEM((NY, 16, TOK), F32),
        pltpu.VMEM((8, TOK), F32),
        pltpu.VMEM((NX, 8, LANE), F32),
        pltpu.VMEM((NZ, 1, TOK), F32),
        pltpu.VMEM((2 * NX * NY, 2, TOK), F32),
        pltpu.SemaphoreType.DMA((LOTS,)),
        pltpu.SemaphoreType.DMA((ARRIVALS,)),
        pltpu.SemaphoreType.DMA((10,)),
    ]
    shapes = (
        jax.ShapeDtypeStruct((TOK, LANE), BF16),
        jax.ShapeDtypeStruct((1, TOK), F32),
        jax.ShapeDtypeStruct((1, LANE), F32),
        jax.ShapeDtypeStruct((1, LANE), F32),
    )
    results = pl.pallas_call(
        kernel,
        name="layer",
        out_shape=shapes,
        in_specs=[hbm] * 10,
        out_specs=(vmem,) * 4,
        scratch_shapes=scratch,
        compiler_params=pltpu.CompilerParams(
            collective_id=0, has_side_effects=True, vmem_limit_bytes=56 * 1024 * 1024
        ),
    )(
        tokens, expert_index.T, slot_index.T, norm_gain[None, :], router_weight,
        final_gain[None, :], gate_weight[0], up_weight[0], down_weight[0], head_weight,
    )
    layer_out, head_logsum, router_penalty, head_penalty = pl.pallas_call(
        finish, name="finish", out_shape=shapes, in_specs=[vmem] * 4, out_specs=(hbm,) * 4,
        scratch_shapes=[pltpu.SemaphoreType.DMA((4,))],
    )(*results)
    return layer_out, head_logsum[0], router_penalty[0, 0], head_penalty[0, 0]


def solution(mesh):
    in_specs = (
        P("dp", ("expert", "mp")),
        P("dp", None),
        P("dp", None),
        P(("expert", "mp")),
        P(None, ("expert", "mp")),
        P("expert", ("dp", "mp"), None),
        P("expert", ("dp", "mp"), None),
        P("expert", ("dp", "mp"), None),
        P(),
        P(("expert", "mp"), None),
    )
    out_specs = (P("dp", ("expert", "mp")), P("dp"), P(), P())
    return jax.shard_map(body, mesh=mesh, in_specs=in_specs, out_specs=out_specs, check_vma=False)
```

```python
import jax
import jax.numpy as jnp
from jax import lax
from jax.experimental import pallas as pl
from jax.experimental.pallas import tpu as pltpu
from jax.sharding import PartitionSpec as P

F32 = jnp.float32
BF16 = jnp.bfloat16
EPSILON = 1e-05
LAST = (((1,), (1,)), ((), ()))
EXACT = lax.Precision.HIGHEST

NX, NY, NZ = 4, 4, 8
CAP = 96
TOK = 256
LANE = 128
HID = 224
HID2 = 2 * HID
WIDTH = LANE * NY * NZ
ROWS = NX * CAP
LOTS = 11
ARRIVALS = 139
CUT_A, CUT_B = 176, 256
SUB_A, SUB_B = 96, 224


class Plan:
    RATE, FIRST, HOP = 46.6e3, 3.1, 0.75

    def __init__(self):
        self.sends, self.works, self.waits, self.given = [], [], {}, {}

    def send(self, group, link, size, needs, emit, hops=1):
        self.sends.append([group, link, size / self.RATE, frozenset(needs), emit, hops])

    def send_both(self, group, axis, size, needs, emit, hops):
        self.send(group, axis + "+", size / 2, needs, emit, hops)
        self.send(group, axis + "-", size / 2, needs, lambda: None, hops)

    def wait(self, group, emit):
        self.waits[group] = emit

    def arrives(self, group, needs, delay, emit):
        self.given[group] = (frozenset(needs), delay)
        self.waits[group] = emit

    def work(self, name, time, needs, emit):
        self.works.append([name, time, frozenset(needs), emit])

    def chains(self):
        after = {}
        for group, _, time, needs, _, hops in self.sends:
            for need in needs:
                after.setdefault(need, []).append(
                    (time + self.FIRST + self.HOP * (hops - 1), group))
        for name, time, needs, _ in self.works:
            for need in needs:
                after.setdefault(need, []).append((time, name))
        for group, (needs, delay) in self.given.items():
            for need in needs:
                after.setdefault(need, []).append((delay, group))
        memo = {}

        def rest(event):
            if event not in memo:
                memo[event] = max((t + rest(n) for t, n in after.get(event, [])), default=0.0)
            return memo[event]

        return rest

    def run(self):
        horizons = (0.3, 0.5, 0.7, 1.0, 1.5)
        return self.play(min(horizons, key=lambda h: self.play(h, False)))

    def play(self, horizon, real=True):
        rest = self.chains()
        clock, free, had = 0.0, {}, set()
        sends, works = list(self.sends), list(self.works)
        left, when, due, done = {}, {}, {}, set()
        for item in sends:
            left[item[0]] = left.get(item[0], 0) + 1

        def issue(force):
            nonlocal sends
            ready = [item for item in sends if item[3] <= had]
            ready.sort(key=lambda item: -(item[2] + rest(item[0])))
            gone = []
            for item in ready:
                group, link, time, _, emit, hops = item
                if free.get(link, 0.0) > clock + horizon and not force:
                    continue
                if real:
                    emit()
                free[link] = max(clock, free.get(link, 0.0)) + time * hops
                arrival = free[link] + self.FIRST + self.HOP * (hops - 1)
                when[group] = max(when.get(group, 0.0), arrival)
                left[group] -= 1
                if left[group] == 0:
                    due[group] = when[group]
                gone.append(id(item))
            sends = [item for item in sends if id(item) not in gone]

        while True:
            for group, (needs, delay) in self.given.items():
                if group not in due and needs <= had:
                    due[group] = clock + delay
            issue(False)
            coming = sorted((time, str(group), group) for group, time in due.items()
                            if group not in done)
            ready = [item for item in works if item[2] <= had]
            ready.sort(key=lambda item: -(item[1] + rest(item[0])))
            chosen = None
            for item in ready:
                if not coming or coming[0][0] - clock >= 0.6 * item[1] or (
                        rest(item[0]) + item[1] > rest(coming[0][2]) + 1.0):
                    chosen = item
                    break
            if chosen is not None:
                works = [item for item in works if item is not chosen]
                if real:
                    chosen[3]()
                clock += chosen[1]
                had.add(chosen[0])
            elif coming:
                time, _, group = coming[0]
                if real:
                    self.waits[group]()
                clock = max(clock, time) + 0.01
                done.add(group)
                had.add(group)
            elif sends:
                issue(True)
            else:
                break
        return clock


def kernel(
    tk_h, ei_h, si_h, ng_h, rw_h, fg_h, gw_h, uw_h, dw_h, hw_h,
    out_ref, lse_ref, rp_ref, hp_ref,
    tk, ei, si, ng, rw, fg,
    w3, hw, ls, xs, acc_g, acc_u, hid, ps, near1, far1,
    sums, near2, far2, fin, rx, chi, clo, hs, acc_h, squares,
    zbuf, ybuf, rbuf, ibuf, mzbuf, mybuf, ssem, rsem, lsem,
):
    d = lax.axis_index("dp")
    e = lax.axis_index("expert")
    m = lax.axis_index("mp")
    x = d // 2
    c = d % 2
    gw, uw, dw = w3.at[0], w3.at[1], w3.at[2]
    coord = {"x": x, "y": m, "z": e}
    extent = {"x": NX, "y": NY, "z": NZ}

    def at(axis, step):
        return (coord[axis] + step + extent[axis]) % extent[axis]

    def device(axis, step):
        if axis == "x":
            return {"dp": at("x", step) * 2 + c, "expert": e, "mp": m}
        if axis == "y":
            return {"dp": d, "expert": e, "mp": at("y", step)}
        return {"dp": d, "expert": at("z", step), "mp": m}

    def plane(step_x, step_y, other):
        dp = at("x", step_x) * 2 + (1 - c if other else c)
        return {"dp": dp, "expert": e, "mp": at("y", step_y)}

    ids = {}
    sent = {}
    lots = {"now": None}
    scopes = []

    def phase(name):
        while scopes:
            scopes.pop().__exit__(None, None, None)
        if name:
            scopes.append(jax.named_scope(name))
            scopes[-1].__enter__()


    def remote(tag, slot, src, dst, dev):
        number = ids.setdefault(tag, len(ids))
        return pltpu.make_async_remote_copy(
            src_ref=src, dst_ref=dst, send_sem=ssem.at[slot], recv_sem=rsem.at[number],
            device_id=dev, device_id_type=pl.DeviceIdType.MESH,
        )

    def send(tag, src, dst, dev):
        lot = lots["now"] or (tag[0] if isinstance(tag, tuple) else tag)
        sent.setdefault(lot, len(sent))
        remote(tag, sent[lot], src, dst, dev).start()

    def send_in(lot, *copy):
        lots["now"] = lot
        send(*copy)
        lots["now"] = None

    def wait(tag, ref):
        remote(tag, 0, ref, ref, device("y", 1)).wait_recv()

    phase("entry")
    smalls = [
        pltpu.make_async_copy(source, held, lsem.at[4 + number])
        for number, (source, held) in enumerate(
            ((tk_h, tk), (ei_h, ei), (si_h, si), (ng_h, ng), (rw_h, rw), (fg_h, fg))
        )
    ]
    loads = [
        pltpu.make_async_copy(gw_h, gw.at[pl.ds(0, HID)], lsem.at[0]),
        pltpu.make_async_copy(uw_h, uw.at[pl.ds(0, HID)], lsem.at[1]),
        pltpu.make_async_copy(dw_h, dw.at[pl.ds(0, HID)], lsem.at[2]),
        pltpu.make_async_copy(hw_h, hw, lsem.at[3]),
    ]
    barrier = pltpu.get_barrier_semaphore()
    partners = [device("z", k) for k in range(1, NZ)]
    others = [
        (step_x, step_y, other)
        for step_x in (2, 1, 3, 0) for step_y in (2, 1, 3, 0) for other in (True, False)
        if (step_x, step_y, other) != (0, 0, False)
    ]
    partners += [plane(*step) for step in others]
    for partner in partners:
        pl.semaphore_signal(
            barrier, inc=1, device_id=partner, device_id_type=pl.DeviceIdType.MESH
        )

    phase("choose")
    for load in smalls + loads:
        load.start()
    for load in smalls:
        load.wait()

    t32 = tk[...].astype(F32)
    gained = (t32 * ng[...]).astype(BF16)
    flat0 = ei[0:1, :] * CAP + si[0:1, :]
    flat1 = ei[1:2, :] * CAP + si[1:2, :]
    slot_iota = lax.broadcasted_iota(jnp.int32, (CAP, TOK), 0)
    for ex in range(NZ):
        rows = slot_iota + ex * CAP
        choose = jnp.where((rows == flat0) | (rows == flat1), 1.0, 0.0).astype(BF16)
        ls[ex] = jnp.dot(choose, gained, preferred_element_type=F32).astype(BF16)
    router_gained = rw[...].astype(F32) * ng[...]
    zbuf[e, 0:8, :] = lax.dot_general(
        router_gained, t32, LAST, precision=EXACT, preferred_element_type=F32
    )
    ones8 = jnp.ones((8, LANE), F32)
    zbuf[e, 8:16, :] = lax.dot_general(
        ones8, t32 * t32, LAST, precision=EXACT, preferred_element_type=F32
    )
    xs[m, x, 0] = ls[e]

    phase("barrier")
    pl.semaphore_wait(barrier, len(partners))
    for k in (1, 7, 2, 6, 3, 5, 4):
        send(("slots", min(k, NZ - k)), ls.at[at("z", k)], xs.at[m, x, NZ - k], device("z", k))
    piece = CAP * LANE * 2
    half = CAP // 2

    def slab(yy, xx, j, part=None):
        if part is None:
            return xs.at[yy, xx, j]
        return xs.at[yy, xx, j, pl.ds(half * part, half)]

    plan = Plan()
    phase("gather")

    def ring(plan, tag, axis, size, views, needs, two, one, last=None):
        end = last or (tag, 2)
        for number, toward in enumerate((1, -1)):
            link = axis + "+-"[number]
            for view in views:
                plan.send((tag, 1), link, size, needs, lambda v=view, w=toward: send_in(
                    "gather", (tag, 1), v(coord[axis]), v(coord[axis]), device(axis, w)))
                plan.send(end, link, size / 2, [(tag, 1)],
                          lambda v=view, w=toward, p=number: send_in(
                    "gather", end, v(at(axis, -w), p), v(at(axis, -w), p), device(axis, w)))
        plan.wait((tag, 1), lambda: wait((tag, 1), two))
        if last is None:
            plan.wait(end, lambda: wait(end, one))

    for k, time in ((1, 3.3), (2, 4.5), (3, 6.0), (4, 7.2)):
        plan.arrives(("slots", k), [], time, lambda k=k: wait(
            ("slots", k), xs.at[m, x, pl.ds(0, 1 if k == 4 else 2)]))
    for j in (0, 7, 1, 6, 2, 5, 3, 4):
        lead, rest = ("x", "y") if j < 4 else ("y", "x")

        def view_of(t, j=j, lead=lead):
            if lead == "x":
                return lambda s, p=None: slab(s, at("x", t), j, p)
            return lambda s, p=None: slab(at("y", t), s, j, p)

        def lead_view(s, p=None, j=j, lead=lead):
            return slab(m, s, j, p) if lead == "x" else slab(s, x, j, p)

        near = [("slots", min(j, NZ - j))] if j > 0 else []
        tag = ("g", j)
        ring(plan, tag, lead, piece, [lead_view], near, xs.at[0, 0, pl.ds(0, 2)], xs.at[0, 0, 0])
        ring(plan, (tag, 0), rest, piece, [view_of(0)], near,
             xs.at[0, 0, pl.ds(0, 2)], None, ("gather end", j in (0, 1, 6, 7)))
        ring(plan, (tag, 1), rest, piece, [view_of(1), view_of(-1)], [(tag, 1)],
             xs.at[0, 0, pl.ds(0, 4)], None, ("gather end", j in (0, 1, 6, 7)))
        ring(plan, (tag, 2), rest, piece, [view_of(2)], [(tag, 2)],
             xs.at[0, 0, pl.ds(0, 2)], None, ("gather end", j in (0, 1, 6, 7)))

    for near in (True, False):
        plan.wait(("gather end", near), lambda n=near: wait(
            ("gather end", n), ps.at[pl.ds(0, 2)]))

    def columns(weight, ex, yy):
        block = (ex % NZ) * NY + yy
        return weight[:, pl.ds(pl.multiple_of(block * LANE, LANE), LANE)]

    def gate_up(yy, pieces):
        held = jnp.concatenate([xs[yy, :, j].reshape(ROWS, LANE) for j in pieces], axis=1)
        for acc, weight in ((acc_g, gw), (acc_u, uw)):
            against = jnp.concatenate([columns(weight, e + j, yy) for j in pieces], axis=1)
            acc[...] += lax.dot_general(held, against, LAST, preferred_element_type=F32)

    def gate_up_rows(steps, pieces):
        blocks = [(yy, j) for yy in range(NY) for j in pieces]
        held = jnp.concatenate([jnp.concatenate(
            [xs[yy, at("x", t), j] for yy, j in blocks], axis=1) for t in steps], axis=0)
        for acc, weight in ((acc_g, gw), (acc_u, uw)):
            against = jnp.concatenate([columns(weight, e + j, yy) for yy, j in blocks], axis=1)
            product = lax.dot_general(held, against, LAST, preferred_element_type=F32)
            for number, t in enumerate(steps):
                rows = pl.ds(pl.multiple_of(at("x", t) * CAP, CAP), CAP)
                acc[rows, :] += product[number * CAP:(number + 1) * CAP]

    def swap_weights():
        for load in loads:
            load.wait()
        send("weights", w3.at[:, pl.ds(0, HID)], w3.at[:, pl.ds(HID, HID)], plane(0, 0, True))

    def router_start():
        for k in range(1, NZ):
            send("router z", zbuf.at[e], zbuf.at[e], device("z", k))

    def router_middle():
        total = zbuf[0]
        for k in range(1, NZ):
            total = total + zbuf[k]
        ybuf[m] = total
        for k in range(1, NY):
            send("router y", ybuf.at[m], ybuf.at[m], device("y", k))

    def router_end():
        total = ((ybuf[0] + ybuf[1]) + ybuf[2]) + ybuf[3]
        inverse8 = lax.rsqrt(total[8:16] / WIDTH + EPSILON)
        rbuf[...] = total[0:8] * inverse8
        place = slot_iota + e * CAP
        mine = jnp.where((place == flat0) | (place == flat1), 1.0, 0.0)
        mine = jnp.concatenate([mine, jnp.zeros((LANE - CAP, TOK), F32)], axis=0)
        ibuf[x] = lax.dot_general(
            inverse8, mine, LAST, precision=EXACT, preferred_element_type=F32
        )
        for k in range(1, NX):
            send("inverse", ibuf.at[x], ibuf.at[x], device("x", k))

    def gates():
        logits = rbuf[...]
        expert_iota = lax.broadcasted_iota(jnp.int32, (8, TOK), 0)
        top = jnp.max(logits, axis=0, keepdims=True)
        mybuf[d * NY + m, 1:2, :] = top + jnp.log(
            jnp.sum(jnp.exp(logits - top), axis=0, keepdims=True))
        picked0 = jnp.sum(jnp.where(expert_iota == ei[0:1, :], logits, 0.0), axis=0, keepdims=True)
        picked1 = jnp.sum(jnp.where(expert_iota == ei[1:2, :], logits, 0.0), axis=0, keepdims=True)
        higher = jnp.maximum(picked0, picked1)
        power0 = jnp.exp(picked0 - higher)
        power1 = jnp.exp(picked1 - higher)
        weight0 = power0 / (power0 + power1)
        weight1 = power1 / (power0 + power1)
        chunk_iota = lax.broadcasted_iota(jnp.int32, (LANE, TOK), 0)
        for j in range(NZ * CAP // LANE):
            rows = chunk_iota + j * LANE
            mixed = jnp.where(rows == flat0, weight0, 0.0) + jnp.where(rows == flat1, weight1, 0.0)
            mixed = mixed.T
            high = mixed.astype(BF16)
            chi[:, j * LANE:(j + 1) * LANE] = high
            clo[:, j * LANE:(j + 1) * LANE] = (mixed - high.astype(F32)).astype(BF16)

    def clear():
        acc_h[...] = jnp.zeros_like(acc_h)
        squares[...] = jnp.zeros_like(squares)
        acc_g[...] = jnp.zeros_like(acc_g)
        acc_u[...] = jnp.zeros_like(acc_u)

    def gain():
        @pl.loop(0, 512 // 16)
        def _(i):
            part = pl.ds(pl.multiple_of(i * 16, 16), 16)
            hw[part, :] = (hw[part, :].astype(F32) * fg[...]).astype(BF16)

    def gate_up_near():
        @pl.loop(0, 2)
        def _(k):
            gate_up((m + 1 + 2 * k) % NY, range(4))

    a_leads = [(("g", j), k) for j in range(4) for k in (1, 2)]
    a_rest = [((("g", j), t), 1) for j in range(4) for t in range(3)]
    plan.work("router start", 0.05, [("slots", 1)], router_start)
    plan.arrives("router z", ["router start"], 6.5, lambda: wait(
        "router z", zbuf.at[pl.ds(0, NZ - 1)]))
    plan.work("swap", 0.1, ["router start"], swap_weights)
    plan.arrives("weights", ["swap"], 12.0, lambda: wait("weights", w3.at[:, pl.ds(HID, HID)]))
    plan.work("router middle", 0.1, ["router z"], router_middle)
    plan.arrives("router y", ["router middle"], 6.0, lambda: wait(
        "router y", ybuf.at[pl.ds(0, NY - 1)]))
    plan.work("router end", 0.4, ["router y"], router_end)
    plan.arrives("inverse", ["router end"], 6.0, lambda: wait(
        "inverse", ibuf.at[pl.ds(0, NX - 1)]))
    plan.work("gates", 0.4, ["router end"], gates)
    plan.work("clear", 0.1, [], clear)
    plan.work("gain", 0.85, ["swap"], gain)
    plan.work("gate up own", 0.72, ["clear", "weights"] + a_leads, lambda: gate_up(m, range(4)))
    plan.work("gate up near", 1.44, ["gate up own"] + a_rest, gate_up_near)
    b_rest = [((("g", j), t), 1) for j in range(4, NZ) for t in range(3)]
    plan.work("gate up rows", 1.3, ["clear", "weights"] + b_rest, lambda: gate_up_rows((0, 1, -1), range(4, NZ)))

    def gate_up_last(near):
        gate_up_rows((2,), (6, 7) if near else (4, 5))
        gate_up(at("y", 2), (0, 1) if near else (2, 3))

    plan.work("gate up last", 0.8, ["clear", "weights", ("gather end", True)]
              + [(("g", j), 2) for j in range(NZ)], lambda: gate_up_last(True))
    plan.run()

    phase("gateup")

    gate_up_last(False)

    for xx in range(NX):
        rows = pl.ds(xx * CAP, CAP)
        scale = jnp.broadcast_to(ibuf[xx, 0:1, :], (LANE, LANE)).T[0:CAP, 0:1]
        gate_value = acc_g[rows, :] * scale
        up_value = acc_u[rows, :] * scale
        hid[rows, :] = (gate_value / (1.0 + jnp.exp(-gate_value)) * up_value).astype(BF16)

    phase("down")
    def down(yy, first):
        against = jnp.concatenate([columns(dw, e + first + j, yy) for j in range(4)], axis=1)
        product = jnp.dot(hid[...], against, preferred_element_type=F32).astype(BF16)
        for j in range(4):
            for xx in range(NX):
                ps[yy * NX + xx, first + j] = product[
                    xx * CAP:(xx + 1) * CAP, j * LANE:(j + 1) * LANE
                ]

    def partial(yy, xx, j, part):
        if part is None:
            return ps.at[yy * NX + xx, j]
        return ps.at[yy * NX + xx, j, pl.ds(half * part, half)]

    def add_into(target, source):
        target[...] = (target[...].astype(F32) + source[...].astype(F32)).astype(BF16)

    plan = Plan()

    def reduce(tag, axis, units, starts, middles, ends):
        names = (tag, 1), (tag, 2)

        def add():
            for view, near, _, _ in units:
                for number, toward in enumerate((1, -1)):
                    add_into(view(at(axis, toward), number), near.at[number])

        def end():
            for view, _, far, into in units:
                into[...] = (view(coord[axis])[...].astype(F32) + far[0].astype(F32)
                             + far[1].astype(F32)).astype(BF16)

        for number, toward in enumerate((1, -1)):
            link = axis + "+-"[number]
            for view, near, far, _ in units:
                plan.send(names[0], link, piece / 2, starts,
                          lambda v=view, n=near, k=number, w=toward: send_in(
                    "reduce", names[0], v(at(axis, 2), k), n.at[k], device(axis, w)))
                plan.send(names[1], link, piece, [(tag, "add")],
                          lambda v=view, f=far, k=number, w=toward: send_in(
                    "reduce", names[1], v(at(axis, w)), f.at[k], device(axis, w)))
        count = len(units)
        plan.wait(names[0], lambda: wait(names[0], ps.at[0, pl.ds(0, count)]))
        plan.wait(names[1], lambda: wait(names[1], ps.at[0, pl.ds(0, 2 * count)]))
        plan.work((tag, "add"), 0.05 * count, [names[0]] + middles, add)
        plan.work((tag, "end"), 0.05 * count, [names[1]] + ends, end)

    def reduce_straight(tag, axis, view, far, into, firsts, seconds, ends):
        def end():
            total = view(coord[axis])[...].astype(F32)
            for number in range(3):
                total = total + far[number].astype(F32)
            into[...] = total.astype(BF16)

        plan.send_both((tag, 2), axis, piece, firsts, lambda: send_in(
                    "reduce", (tag, 2), view(at(axis, 2)), far.at[2], device(axis, 2)), 2)
        for number, toward in enumerate((1, -1)):
            plan.send((tag, 2), axis + "+-"[number], piece, seconds,
                      lambda k=number, w=toward: send_in(
                    "reduce", (tag, 2), view(at(axis, w)), far.at[k], device(axis, w)))
        plan.wait((tag, 2), lambda: wait((tag, 2), ps.at[0, pl.ds(0, 3)]))
        plan.work((tag, "end"), 0.05, [(tag, 2)] + ends, end)

    for j in (0, 1, 2, 3, 4, 5, 6, 7):
        lead, rest = ("y", "x") if j < 4 else ("x", "y")

        def unit_of(t, j=j, lead=lead, rest=rest):
            if lead == "y":
                view = lambda s, p=None: partial(s, at("x", t), j, p)
            else:
                view = lambda s, p=None: partial(at("y", t), s, j, p)
            return view, near1.at[j, t % 4], far1.at[j, t % 4], sums.at[j, at(rest, t)]

        def sum_view(s, p=None, j=j):
            return sums.at[j, s] if p is None else sums.at[j, s, pl.ds(half * p, half)]

        for t, steps in ((2, (2,)), (1, (1, -1)), (0, (0,))):
            if lead == "y":
                starts, middles, ends = [("down", 0, 2)], [("down", 0, 1), ("down", 0, 3)], [
                    ("down", 0, 0)]
            else:
                starts = [("down", 4, step % 4) for step in steps]
                middles, ends = [], []
            reduce(("r", j, t), lead, [unit_of(step) for step in steps], starts, middles, ends)
        last = [[(("r", j, t), "end")] for t in (2, 1, 0)]
        if j in (0, 1, 6, 7):
            reduce_straight(("s", j), rest, sum_view, far2.at[j], fin.at[j], *last)
        else:
            reduce(("s", j), rest, [(sum_view, near2.at[j], far2.at[j], fin.at[j])], *last)
        if j > 0:
            hops = min(j, NZ - j)
            back = lambda j=j: send("back", fin.at[j], rx.at[e], device("z", j))
            if j == 4:
                plan.send_both("back", "z", piece, [(("s", j), "end")], back, hops)
            else:
                plan.send("back", "z+" if j < 4 else "z-", piece, [(("s", j), "end")], back, hops)
    plan.wait("back", lambda: wait("back", rx.at[pl.ds(0, NZ - 1)]))
    for first, step in ((0, 2), (4, 2), (4, 1), (4, 3), (0, 1), (0, 3), (4, 0), (0, 0)):
        plan.work(("down", first, step), 0.45, [],
                  lambda f=first, t=step: down(at("y", t), f))
    plan.run()
    phase("back")
    rx[e] = fin[0]
    phase("combine")
    outputs = rx[...].reshape(NZ * CAP, LANE)
    combined = jnp.dot(chi[...], outputs, preferred_element_type=F32)
    combined += jnp.dot(clo[...], outputs, preferred_element_type=F32)
    layer_out = (tk[...].astype(F32) + combined).astype(BF16)
    out_ref[...] = layer_out
    hs[m * NZ + e] = layer_out

    phase("head_gather")
    def rows_a(yy, zz, part=None):
        if part is None:
            return hs.at[yy * NZ + zz, pl.ds(0, CUT_A)]
        return hs.at[yy * NZ + zz, pl.ds(0, SUB_A)] if part == 0 else hs.at[
            yy * NZ + zz, pl.ds(SUB_A, CUT_A - SUB_A)]

    def rows_b(yy, zz, part=None):
        if part is None:
            return hs.at[yy * NZ + zz, pl.ds(CUT_A, CUT_B - CUT_A)]
        return hs.at[yy * NZ + zz, pl.ds(CUT_A, SUB_B - CUT_A)] if part == 0 else hs.at[
            yy * NZ + zz, pl.ds(SUB_B, CUT_B - SUB_B)]

    def ring8(rounds, start, tag, view, times):
        def begin():
            for k in (2, 1):
                for toward in (1, -1):
                    send_in("head", (tag, k), view(e), view(e), device("z", toward * k))

        def step():
            wait((tag, 2), times(2))
            for toward, part in ((1, 0), (-1, 1)):
                source = at("z", -toward * 2)
                unit = view(source, part)
                send_in("head", (tag, 3), unit, unit, device("z", toward * 2))
                send_in("head", (tag, 3), view(source), view(source), device("z", toward))
            wait((tag, 1), times(2))

        def finish():
            wait((tag, 3), times(3))

        for number, event in enumerate((begin, step, finish)):
            rounds.setdefault(start + number, []).append(event)

    def logits_chunk(yy):
        held = jnp.concatenate([hs[yy * NZ + zz] for zz in range(NZ)], axis=1)
        against = jnp.concatenate([columns(hw, zz, yy) for zz in range(NZ)], axis=1)
        acc_h[...] += lax.dot_general(against, held, LAST, preferred_element_type=F32)
        total = squares[...]
        for zz in range(NZ):
            block = hs[yy * NZ + zz].astype(F32)
            total = total + block * block
        squares[...] = total

    def play(rounds, number):
        for event in rounds.get(number, []):
            event()

    def ring4(rounds, start, tag, axis, view, two, last=None):
        def begin():
            for toward in (1, -1):
                send_in("head", (tag, 1), view(coord[axis]), view(coord[axis]), device(axis, toward))

        def step():
            wait((tag, 1), two)
            for toward, part in ((1, 0), (-1, 1)):
                unit = view(at(axis, -toward), part)
                send_in("head", last or (tag, 2), unit, unit, device(axis, toward))

        def finish():
            if last is None:
                wait((tag, 2), view(at(axis, 2)))

        for number, event in enumerate((begin, step, finish)):
            rounds.setdefault(start + number, []).append(event)

    head = {}
    ring4(head, 0, "hb y", "y", lambda s, p=None: rows_b(s, e, p),
         hs.at[pl.ds(0, 2), pl.ds(CUT_A, CUT_B - CUT_A)])
    ring8(head, 0, "ha z", lambda s, p=None: rows_a(m, s, p),
          lambda n: hs.at[pl.ds(0, n), pl.ds(0, CUT_A)])
    for start, near, far in ((2, (3, -3, 4), (2,)), (1, (1, -1, 2, -2), (1, -1)), (0, (0,), (0,))):
        for t in far:
            ring8(head, start, ("hb z", t), lambda s, p=None, t=t: rows_b(at("y", t), s, p),
                  lambda n, t=t: hs.at[pl.ds(0, n), pl.ds(CUT_A, CUT_B - CUT_A)])
        for t in near:
            ring4(head, start, ("ha y", t), "y", lambda s, p=None, t=t: rows_a(s, at("z", t), p),
                 hs.at[pl.ds(0, 2), pl.ds(0, CUT_A)], "ha end")
    play(head, 0)
    play(head, 1)
    play(head, 2)

    logits_chunk(m)
    play(head, 3)

    @pl.loop(0, 2)
    def _(k):
        logits_chunk((m + 1 + 2 * k) % NY)

    play(head, 4)
    wait("ha end", hs.at[pl.ds(0, NZ), pl.ds(0, CUT_A)])
    phase("logits")
    logits_chunk(at("y", 2))
    high = squares[...].astype(BF16)
    low = (squares[...] - high.astype(F32)).astype(BF16)
    ones16 = jnp.ones((16, LANE), BF16)
    total = lax.dot_general(ones16, high, LAST, preferred_element_type=F32)
    total += lax.dot_general(ones16, low, LAST, preferred_element_type=F32)
    head_scale = lax.rsqrt(total[0:1, :] / WIDTH + EPSILON)
    vocab = acc_h[...] * head_scale

    def logsum(rows):
        top = jnp.max(rows, axis=0, keepdims=True)
        return top + jnp.log(jnp.sum(jnp.exp(rows - top), axis=0, keepdims=True))

    def merged(rows):
        top = rows[0]
        for row in rows[1:]:
            top = jnp.maximum(top, row)
        whole = jnp.exp(rows[0] - top)
        for row in rows[1:]:
            whole = whole + jnp.exp(row - top)
        return top + jnp.log(whole)

    mzbuf[e] = logsum(vocab)
    phase("merge_z")
    for k in (4, 3, 5, 2, 6, 1, 7):
        send("merge z", mzbuf.at[e], mzbuf.at[e], device("z", k))
    wait("merge z", mzbuf.at[pl.ds(0, NZ - 1)])
    mybuf[d * NY + m, 0:1, :] = merged([mzbuf[k] for k in range(NZ)])
    phase("merge_xy")
    for step in others:
        send("merge xy", mybuf.at[d * NY + m], mybuf.at[d * NY + m], plane(*step))
    wait("merge xy", mybuf.at[pl.ds(0, len(others))])
    phase("penalty")
    router_sum = jnp.zeros((1, TOK), F32)
    head_sum = jnp.zeros((1, TOK), F32)
    for dp in range(2 * NX):
        routed = mybuf[dp * NY, 1:2, :]
        router_sum = router_sum + routed * routed
        ended = merged([mybuf[dp * NY + yy, 0:1, :] for yy in range(NY)])
        head_sum = head_sum + ended * ended
    lse_ref[...] = merged([mybuf[d * NY + yy, 0:1, :] for yy in range(NY)])

    def spread(row):
        return jnp.broadcast_to(jnp.sum(row, axis=1, keepdims=True), (1, LANE))

    rp_ref[...] = spread(router_sum) / (2 * NX * TOK)
    hp_ref[...] = spread(head_sum) / (2 * NX * TOK)

    phase("drain")
    for lot, ref in (
        ("slots", ls.at[pl.ds(0, NZ - 1)]), ("router z", zbuf.at[pl.ds(0, NZ - 1)]),
        ("weights", w3.at[:, pl.ds(0, HID)]), ("router y", ybuf.at[pl.ds(0, NY - 1)]),
        ("inverse", ibuf.at[pl.ds(0, NX - 1)]), ("gather", ps.at[pl.ds(0, NX * NY - 1)]),
        ("reduce", ps.at[pl.ds(0, NX * NY - 1)]), ("back", fin.at[pl.ds(0, NZ - 1)]),
        ("head", hs.at[pl.ds(0, NY * NZ - 1)]), ("merge z", mzbuf.at[pl.ds(0, NZ - 1)]),
        ("merge xy", mybuf.at[pl.ds(0, len(others))]),
    ):
        remote(("slots", 1), sent[lot], ref, ref, device("y", 1)).wait_send()
    phase("")
    assert len(ids) == ARRIVALS and len(sent) == LOTS, (len(ids), len(sent))


def finish(*refs):
    sources, results, sem = refs[:4], refs[4:8], refs[8]
    copies = [pltpu.make_async_copy(source, result, sem.at[number])
              for number, (source, result) in enumerate(zip(sources, results))]
    for copy in copies:
        copy.start()
    for copy in copies:
        copy.wait()


def body(tokens, expert_index, slot_index, norm_gain, router_weight, gate_weight, up_weight,
         down_weight, final_gain, head_weight):
    vmem = pl.BlockSpec(memory_space=pltpu.VMEM)
    hbm = pl.BlockSpec(memory_space=pl.ANY)
    scratch = [
        pltpu.VMEM((TOK, LANE), BF16),
        pltpu.VMEM((2, TOK), jnp.int32),
        pltpu.VMEM((2, TOK), jnp.int32),
        pltpu.VMEM((1, LANE), F32),
        pltpu.VMEM((8, LANE), BF16),
        pltpu.VMEM((1, WIDTH), F32),
        pltpu.VMEM((3, HID2, WIDTH), BF16),
        pltpu.VMEM((512, WIDTH), BF16),
        pltpu.VMEM((NZ, CAP, LANE), BF16),
        pltpu.VMEM((NY, NX, NZ, CAP, LANE), BF16),
        pltpu.VMEM((ROWS, HID2), F32),
        pltpu.VMEM((ROWS, HID2), F32),
        pltpu.VMEM((ROWS, HID2), BF16),
        pltpu.VMEM((NY * NX, NZ, CAP, LANE), BF16),
        pltpu.VMEM((NZ, 4, 2, CAP // 2, LANE), BF16),
        pltpu.VMEM((NZ, 4, 2, CAP, LANE), BF16),
        pltpu.VMEM((NZ, 4, CAP, LANE), BF16),
        pltpu.VMEM((NZ, 2, CAP // 2, LANE), BF16),
        pltpu.VMEM((NZ, 3, CAP, LANE), BF16),
        pltpu.VMEM((NZ, CAP, LANE), BF16),
        pltpu.VMEM((NZ, CAP, LANE), BF16),
        pltpu.VMEM((TOK, NZ * CAP), BF16),
        pltpu.VMEM((TOK, NZ * CAP), BF16),
        pltpu.VMEM((NY * NZ, TOK, LANE), BF16),
        pltpu.VMEM((512, TOK), F32),
        pltpu.VMEM((TOK, LANE), F32),
        pltpu.VMEM((NZ, 16, TOK), F32),
        pltpu.VMEM((NY, 16, TOK), F32),
        pltpu.VMEM((8, TOK), F32),
        pltpu.VMEM((NX, 8, LANE), F32),
        pltpu.VMEM((NZ, 1, TOK), F32),
        pltpu.VMEM((2 * NX * NY, 2, TOK), F32),
        pltpu.SemaphoreType.DMA((LOTS,)),
        pltpu.SemaphoreType.DMA((ARRIVALS,)),
        pltpu.SemaphoreType.DMA((10,)),
    ]
    shapes = (
        jax.ShapeDtypeStruct((TOK, LANE), BF16),
        jax.ShapeDtypeStruct((1, TOK), F32),
        jax.ShapeDtypeStruct((1, LANE), F32),
        jax.ShapeDtypeStruct((1, LANE), F32),
    )
    results = pl.pallas_call(
        kernel,
        name="layer",
        out_shape=shapes,
        in_specs=[hbm] * 10,
        out_specs=(vmem,) * 4,
        scratch_shapes=scratch,
        compiler_params=pltpu.CompilerParams(
            collective_id=0, has_side_effects=True, vmem_limit_bytes=56 * 1024 * 1024
        ),
    )(
        tokens, expert_index.T, slot_index.T, norm_gain[None, :], router_weight,
        final_gain[None, :], gate_weight[0], up_weight[0], down_weight[0], head_weight,
    )
    layer_out, head_logsum, router_penalty, head_penalty = pl.pallas_call(
        finish, name="finish", out_shape=shapes, in_specs=[vmem] * 4, out_specs=(hbm,) * 4,
        scratch_shapes=[pltpu.SemaphoreType.DMA((4,))],
    )(*results)
    return layer_out, head_logsum[0], router_penalty[0, 0], head_penalty[0, 0]


def solution(mesh):
    in_specs = (
        P("dp", ("expert", "mp")),
        P("dp", None),
        P("dp", None),
        P(("expert", "mp")),
        P(None, ("expert", "mp")),
        P("expert", ("dp", "mp"), None),
        P("expert", ("dp", "mp"), None),
        P("expert", ("dp", "mp"), None),
        P(),
        P(("expert", "mp"), None),
    )
    out_specs = (P("dp", ("expert", "mp")), P("dp"), P(), P())
    return jax.shard_map(body, mesh=mesh, in_specs=in_specs, out_specs=out_specs, check_vma=False)
```
